32 devices in a mesh: seq: 4 (over z), head: 4 (over y, x), batch: 2 (over core).
Axes of the slice: x: 2, y: 2, z: 4, core: 2. Of those that a mesh axis runs over, the one named last changes fastest.
Arguments:
- tokens: bfloat16 [4096, 2560], P(('batch', 'seq'), 'head'), parts along dimension 0, may hold values from -6 to 6
- resets: int32 [4096], P(('batch', 'seq')), parts along dimension 0, may hold values 0 or 1
- w_x: bfloat16 [2560, 5120], P(None, 'head'), may hold values from -0.125 to 0.125
- w_z: bfloat16 [2560, 5120], P(None, 'head'), may hold values from -0.125 to 0.125
- w_bc: bfloat16 [2560, 256], replicated, may hold values from -0.125 to 0.125
- w_dt: bfloat16 [2560, 80], P(None, 'head'), may hold values from -0.125 to 0.125
- dt_bias: float32 [80], P('head'), may hold values from -2 to 1
- decay_rate: float32 [80], P('head'), may hold values from 0.00024414062 to 0.08
- d_skip: float32 [80], P('head'), may hold values from 0.5 to 1.5
- norm_gain: float32 [5120], P('head'), may hold values from 0.5 to 1.5
- w_out: bfloat16 [5120, 2560], P('head'), may hold values from -0.078125 to 0.078125
Outputs:
- mixed: bfloat16 [4096, 2560], P(('batch', 'seq'), 'head'), parts along dimension 0
The draws below stay inside these ranges and needn't reach their ends.
There are 2 independent parts, one for each index of `batch`. The reference program is written for one: setup_inputs(seed, part) draws one part's arguments, and reference() takes and returns one part's arrays. A program takes and returns all parts, laid end to end along the dimension named above; an argument that names none is the same for every part. Nothing has to cross between parts.
All inputs are finite; a program needn't handle non-finite values. No bound on the sum of `resets` on one device may be relied on, other than what follows from the above.
Results may differ from the reference program's by a relative error of at most 0.013.
Values may be sent and summed in bfloat16 or wider, within the bound.
A program may use at most 128 MiB of HBM per device.

```python
import math
import jax
import jax.numpy as jnp
from jax import lax

D = 2560
DI = 5120
HEADS = 80
HEADDIM = 64
NSTATE = 128
L_DEV = 512
GROUP = 256
LENGTH = 2048


def with_ends(array, own_key, smallest, high):
    longest = array.shape.index(max(array.shape))
    spots = []
    for shift in (0, 1):
        where = [jax.random.randint(jax.random.fold_in(own_key, axis), (), 0, length) for axis, length in enumerate(array.shape)]
        where[longest] = (where[longest] + shift) % array.shape[longest]
        spots.append(tuple(where))
    return array.at[spots[0]].set(smallest).at[spots[1]].set(high)


def level_of(stream_key, extent, cuts, least, high):
    level, own = 1.0, jax.random.fold_in(stream_key, 6)
    for dim, shards_of in cuts:
        heights = jnp.exp(jax.random.uniform(jax.random.fold_in(own, dim), (shards_of,), jnp.float32, least / len(cuts), high / len(cuts)))
        level = level * jnp.repeat(heights, extent[dim] // shards_of).reshape([-1 if axis == dim else 1 for axis in range(len(extent))])
    return level


def normal_values(own_key, dims, scale, most, split=(), kind=jnp.bfloat16):
    result = scale * jax.random.normal(own_key, dims, jnp.float32)
    if split:
        result = result * level_of(own_key, dims, split, -0.22, 0.18)
    return jnp.clip(result, -most, most).astype(kind)


def setup_inputs(seed: int = 0, part: int = 0) -> dict:
    keys = jax.random.split(jax.random.key(seed), 12)
    part_splits = jax.random.split(jax.random.fold_in(keys[11], part), 12)
    tokens = normal_values(part_splits[0], (LENGTH, D), 1.0, 6.0, ((0, 4), (1, 4)))
    resets = with_ends((jax.random.randint(part_splits[1], (LENGTH,), 0, 2 * L_DEV) < 1).astype(jnp.int32), jax.random.fold_in(part_splits[1], 1), 0, 1)
    w_x = normal_values(keys[2], (D, DI), D ** -0.5, 0.125, ((1, 4),))
    w_z = normal_values(keys[3], (D, DI), D ** -0.5, 0.125, ((1, 4),))
    w_bc = normal_values(keys[4], (D, 2 * NSTATE), D ** -0.5, 0.125)
    w_dt = normal_values(keys[5], (D, HEADS), D ** -0.5, 0.125, ((1, 4),))
    dt_bias = jnp.clip(-2.0 + 3.0 * jax.random.uniform(keys[6], (HEADS,), jnp.float32) ** level_of(keys[6], (HEADS,), ((0, 4),), -0.2, 0.2), -2.0, 1.0)
    decay_rate = jnp.clip(jnp.exp(math.log(0.08) - 5.7920375 * jax.random.uniform(keys[7], (HEADS,), jnp.float32) ** level_of(keys[7], (HEADS,), ((0, 4),), -0.2, 0.2)), 0.00024414062, 0.08)
    d_skip = jnp.clip(0.5 + 1.0 * jax.random.uniform(keys[8], (HEADS,), jnp.float32) ** level_of(keys[8], (HEADS,), ((0, 4),), -0.2, 0.2), 0.5, 1.5)
    norm_gain = jnp.clip(1.0 + 0.1 * jax.random.normal(keys[9], (DI,), jnp.float32), 0.5, 1.5)
    w_out = normal_values(keys[10], (DI, D), DI ** -0.5, 0.078125, ((0, 4),))
    return {"tokens": tokens, "resets": resets, "w_x": w_x, "w_z": w_z, "w_bc": w_bc, "w_dt": w_dt, "dt_bias": dt_bias, "decay_rate": decay_rate, "d_skip": d_skip, "norm_gain": norm_gain, "w_out": w_out}


def decay_block(inputs, step_size, log_decay, in_proj, out_proj, restart, state_in):
    cumulative = jnp.cumsum(log_decay, axis=0)
    segment = jnp.cumsum(restart)
    places = jnp.arange(restart.shape[0], dtype=jnp.int32)
    same_doc = (segment[:, None] == segment[None, :]) & (places[:, None] >= places[None, :])
    scores = jnp.dot(out_proj, in_proj.T, preferred_element_type=jnp.float32)
    spread = cumulative.T[:, :, None] - cumulative.T[:, None, :]
    factor = jnp.exp(jnp.where(same_doc[None], spread, -jnp.inf))
    mixing = (factor * scores[None] * step_size.T[:, None, :]).astype(jnp.bfloat16)
    output = jnp.einsum('hts,shp->thp', mixing.astype(jnp.float32), inputs.astype(jnp.float32))
    entering = jnp.where((segment == 0)[:, None], jnp.exp(cumulative), 0.0)
    carried = jnp.einsum('tn,hpn->thp', out_proj.astype(jnp.float32), state_in, precision=lax.Precision.HIGHEST)
    output = output + entering[:, :, None] * carried
    closing = segment[-1]
    keeping = jnp.where((segment == closing)[:, None], jnp.exp(cumulative[-1][None, :] - cumulative), 0.0) * step_size
    scaled = (keeping[:, :, None] * inputs.astype(jnp.float32)).astype(jnp.bfloat16)
    update = jnp.einsum('shp,sn->hpn', scaled.astype(jnp.float32), in_proj.astype(jnp.float32))
    through = jnp.where(closing == 0, jnp.exp(cumulative[-1]), 0.0)
    return (output, update + through[:, None, None] * state_in)

def reference(tokens, resets, w_x, w_z, w_bc, w_dt, dt_bias, decay_rate, d_skip, norm_gain, w_out):
    inner = jax.nn.silu(jnp.dot(tokens, w_x, preferred_element_type=jnp.float32)).astype(jnp.bfloat16)
    gating = jnp.dot(tokens, w_z, preferred_element_type=jnp.float32).astype(jnp.bfloat16)
    mapped = jax.nn.silu(jnp.dot(tokens, w_bc, preferred_element_type=jnp.float32)).astype(jnp.bfloat16)
    step_size = jax.nn.softplus(jnp.dot(tokens, w_dt, preferred_element_type=jnp.float32) + dt_bias)
    log_decay = -step_size * decay_rate
    blocks = LENGTH // GROUP
    sliced = (inner.reshape(blocks, GROUP, HEADS, HEADDIM), step_size.reshape(blocks, GROUP, HEADS), log_decay.reshape(blocks, GROUP, HEADS), mapped[:, :NSTATE].reshape(blocks, GROUP, NSTATE), mapped[:, NSTATE:].reshape(blocks, GROUP, NSTATE), resets.reshape(blocks, GROUP))

    def advance(state_in, pieces):
        output, state_out = decay_block(pieces[0], pieces[1], pieces[2], pieces[3], pieces[4], pieces[5], state_in)
        return (state_out, output)
    final_state, outputs = lax.scan(advance, jnp.zeros((HEADS, HEADDIM, NSTATE), jnp.float32), sliced)
    mixed_heads = outputs.reshape(LENGTH, HEADS, HEADDIM) + d_skip[None, :, None] * inner.reshape(LENGTH, HEADS, HEADDIM).astype(jnp.float32)
    gated = mixed_heads.reshape(LENGTH, DI) * jax.nn.silu(gating.astype(jnp.float32))
    meansq = lax.optimization_barrier(jnp.mean(gated * gated, axis=1, keepdims=True))
    normed = (gated * lax.rsqrt(meansq + 1e-05) * norm_gain).astype(jnp.bfloat16)
    return jnp.dot(normed, w_out, preferred_element_type=jnp.float32).astype(jnp.bfloat16)
```

```python
import functools
import math

import jax
import jax.numpy as jnp
from jax import lax
from jax.experimental import pallas as pl
from jax.experimental.pallas import tpu as pltpu
from jax.sharding import PartitionSpec as P

HEADDIM = 64
NSTATE = 128
GROUP = 256
LANES = 128
CHUNK = 128
WIDE = 256
F32 = jnp.float32
BF16 = jnp.bfloat16
MESH = pl.DeviceIdType.MESH
ANY = pl.BlockSpec(memory_space=pl.ANY)
EPS = 1e-05
LOG2E = math.log2(math.e)


def peers():
    me = lax.axis_index("head")
    across = me + 1 - 2 * lax.rem(me, 2)
    along = lax.rem(me + 2, 4)
    corner = lax.rem(across + 2, 4)
    return me, across, along, corner


def remote(axis, to, src, dst, send, recv):
    return pltpu.make_async_remote_copy(
        src_ref=src, dst_ref=dst, send_sem=send, recv_sem=recv, device_id={axis: to}, device_id_type=MESH
    )


def silu(v):
    return v / (1.0 + jnp.exp(-v))


class Scratch:
    def __init__(self, names, refs):
        for name, ref in zip(names, refs):
            setattr(self, name, ref)


def dot(a, b):
    return jnp.dot(a, b, preferred_element_type=F32)


def dot_nt(a, b, precision=None):
    return lax.dot_general(a, b, (((1,), (1,)), ((), ())), preferred_element_type=F32, precision=precision)


def two_terms(v):
    high = v.astype(BF16)
    return jnp.concatenate([high, (v - high.astype(F32)).astype(BF16)], axis=1)


def kernel(chain, total, names, tok, resets, w_x, w_z, w_bc, w_dt, bias, rate, skip, gain, w_out, out, *refs):
    r = Scratch(names, refs)
    me, across, along, corner = peers()
    pos = lax.axis_index("seq")
    upper, lower = lax.rem(pos + 1, chain), lax.rem(pos + chain - 1, chain)
    rows, depth = tok.shape
    width = w_x.shape[1]
    heads = w_dt.shape[0]
    blocks, pairs, per = rows // GROUP, width // LANES, LANES // HEADDIM
    half = GROUP // 2
    chunks, parts = rows // CHUNK, GROUP // CHUNK
    first = 3 * depth // WIDE * WIDE
    owners = (me, across, along, corner)
    tiles = [slice(i, min(i + WIDE, width)) for i in range(0, width, WIDE)]

    def span_of(owner):
        return pl.ds(pl.multiple_of(owner * depth, LANES), depth)

    def place(k):
        return slice(k * depth, (k + 1) * depth)

    def rows_of(b):
        return slice(b * GROUP, (b + 1) * GROUP)

    def chunk_rows(i):
        return slice(i * CHUNK, (i + 1) * CHUNK)

    own_tokens = pltpu.make_async_copy(tok, r.xt.at[:, place(0)], r.small_load.at[0])
    own_tokens.start()
    barrier = pltpu.get_barrier_semaphore()
    for other in (across, along):
        pl.semaphore_signal(barrier, inc=1, device_id={"head": other}, device_id_type=MESH)
    for other in (upper, lower):
        pl.semaphore_signal(barrier, inc=1, device_id={"seq": other}, device_id_type=MESH)
    smalls = [
        pltpu.make_async_copy(src, dst, r.small_load.at[1 + i])
        for i, (src, dst) in enumerate(
            (
                (resets, r.resets), (w_dt, r.w_dt), (bias, r.bias0), (rate, r.rate0), (skip, r.skip0), (gain, r.gain),
            )
        )
    ]
    for copy in smalls:
        copy.start()
    loads = [
        (
            pltpu.make_async_copy(w_x.at[span_of(owner)], r.vx.at[place(k)], r.load.at[3 * k]),
            pltpu.make_async_copy(w_z.at[span_of(owner)], r.vz.at[place(k)], r.load.at[3 * k + 1]),
            pltpu.make_async_copy(w_bc.at[span_of(owner)], r.vb.at[place(k)], r.load.at[3 * k + 2]),
        )
        for k, owner in enumerate(owners)
    ]
    order = (corner, across, along, me)
    out_loads = [
        pltpu.make_async_copy(w_out.at[:, span_of(owner)], r.vw.at[k], r.load_out.at[k])
        for k, owner in enumerate(order)
    ]
    for group in loads:
        for copy in group:
            copy.start()

    gathers = []
    for b in range(blocks):
        lo = slice(b * GROUP, b * GROUP + half)
        hi = slice(b * GROUP + half, (b + 1) * GROUP)
        plan = (
            (across, r.xt.at[lo, place(0)], r.xt.at[lo, place(1)]),
            (along, r.xt.at[hi, place(0)], r.xt.at[hi, place(2)]),
            (across, r.xt.at[hi, place(0)], r.xt.at[hi, place(1)]),
            (along, r.xt.at[lo, place(0)], r.xt.at[lo, place(2)]),
            (along, r.xt.at[lo, place(1)], r.xt.at[lo, place(3)]),
            (across, r.xt.at[hi, place(2)], r.xt.at[hi, place(3)]),
        )
        gathers.append([
            remote("head", to, src, dst, r.g_send.at[6 * b + i], r.g_recv.at[6 * b + i])
            for i, (to, src, dst) in enumerate(plan)
        ])
    own_tokens.wait()
    pl.semaphore_wait(barrier, 4)
    for copy in gathers[0][:4]:
        copy.start()

    ti = lax.broadcasted_iota(jnp.int32, (CHUNK, CHUNK), 0)
    si = lax.broadcasted_iota(jnp.int32, (CHUNK, CHUNK), 1)
    causal = ti >= si
    tri = jnp.where(causal, 1.0, 0.0).astype(F32)
    left = si < HEADDIM
    for k in range(3):
        r.tri[:, k * CHUNK : (k + 1) * CHUNK] = tri.astype(BF16)
    for cols in tiles:
        shape = (2 * LANES, cols.stop - cols.start)
        channel = lax.broadcasted_iota(jnp.int32, shape, 1) + cols.start
        source = lax.rem(lax.broadcasted_iota(jnp.int32, shape, 0), LANES)
        inside = (channel >= source * HEADDIM) & (channel < (source + 1) * HEADDIM)
        r.widen[:, cols] = jnp.where(inside, 1.0, 0.0).astype(BF16)
    for copy in smalls:
        copy.wait()
    r.rate[...] = jnp.zeros_like(r.rate)
    r.rate[:, :heads] = r.rate0[...] * LOG2E
    r.bias[...] = jnp.zeros_like(r.bias)
    r.bias[:, :heads] = r.bias0[...]
    r.skip[...] = jnp.zeros_like(r.skip)
    r.skip[:, :heads] = r.skip0[...]
    r.wd[...] = jnp.zeros_like(r.wd)
    for k, owner in enumerate(owners):
        r.wd[:heads, place(k)] = r.w_dt[:, span_of(owner)]
    spare = jnp.broadcast_to(r.skip[...], (8, LANES))
    for cols in tiles:
        r.skips[:, cols] = dot(two_terms(spare), r.widen[:, cols])
    seen = jnp.zeros((1, LANES), F32)
    for i in range(chunks):
        rs = chunk_rows(i)
        starts = r.resets[:, rs].astype(F32)
        seg = jnp.broadcast_to(jnp.sum(tri * starts, axis=1, keepdims=True), (CHUNK, CHUNK))
        last = seg[CHUNK - 1 :, :]
        r.mask[i] = jnp.where(causal & (seg == seg.T), 1.0, 0.0)
        r.alone[rs, :] = jnp.where(seg == 0.0, 1.0, 0.0)
        r.same[rs, :] = jnp.where(seg == last, 1.0, 0.0)
        r.open[rs, :] = jnp.where(seg + seen == 0.0, 1.0, 0.0)
        seen = seen + last

    def early(b, which):
        rs = rows_of(b)
        x = r.xt.at[rs, :first]
        if "x" in which:
            for cols in tiles:
                r.acc_x[:, cols] = dot(x[...], r.vx[:first, cols])
            r.acc_m[...] = dot(x[...], r.vb[:first, :])
            r.acc_s[...] = dot_nt(x[...], r.wd[:, :first])
        if "z" in which:
            for cols in tiles:
                r.acc_z[:, cols] = dot(x[...], r.vz[:first, cols])

    def late_small(b):
        rs = rows_of(b)
        x = r.xt.at[rs, first:]
        r.mapped[rs, :] = silu(r.acc_m[...] + dot(x[...], r.vb[first:, :])).astype(BF16)
        v = r.acc_s[...] + dot_nt(x[...], r.wd[:, first:]) + r.bias[...]
        r.step[...] = jnp.maximum(v, 0.0) + jnp.log1p(jnp.exp(-jnp.abs(v)))

    def late_x(b):
        rs = rows_of(b)
        x = r.xt.at[rs, first:]
        for cols in tiles:
            r.inner[rs, cols] = silu(r.acc_x[:, cols] + dot(x[...], r.vx[first:, cols])).astype(BF16)

    def late_z(b):
        rs = rows_of(b)
        x = r.xt.at[rs, first:]
        for cols in tiles:
            z = (r.acc_z[:, cols] + dot(x[...], r.vz[first:, cols])).astype(BF16).astype(F32)
            r.gate[rs, cols] = silu(z)

    def prepare(b):
        for i in range(b * parts, (b + 1) * parts):
            rs = chunk_rows(i)
            stp = r.step[(i - b * parts) * CHUNK : (i - b * parts + 1) * CHUNK, :]
            decay = -stp * r.rate[...]
            high = decay.astype(BF16)
            rest = decay - high.astype(F32)
            middle = rest.astype(BF16)
            low = (rest - middle.astype(F32)).astype(BF16)
            cum = dot(r.tri[...], jnp.concatenate([high, middle, low], axis=0))
            last = cum[CHUNK - 1 :, :]
            before = r.before[i : i + 1, :]
            r.before[i + 1 : i + 2, :] = before + last
            r.cum[i] = cum
            r.cumt[i] = cum.T
            r.stept[i] = stp.T
            r.keep[rs, :] = two_terms(r.same[rs, :] * jnp.exp2(last - cum) * stp)
            r.enter[rs, :] = two_terms(r.alone[rs, :] * jnp.exp2(cum))
            r.outer[rs, :] = two_terms(r.open[rs, :] * jnp.exp2(before + cum))
            mapped_b, mapped_c = r.mapped[rs, :NSTATE], r.mapped[rs, NSTATE:]
            r.score[i] = r.mask[i] * dot_nt(mapped_c, mapped_b)
            r.turned[i] = mapped_b.astype(F32).T.astype(BF16)

    def down(c):
        return remote("seq", upper, r.leaving.at[c], r.arrived.at[c], r.c_send.at[c], r.c_recv.at[c])

    def states(i):
        rs = chunk_rows(i)
        for cols in tiles:
            scaled = (dot(r.keep[rs, :], r.widen[:, cols]) * r.inner[rs, cols].astype(F32)).astype(BF16)
            new = dot(r.turned[i], scaled)
            if i:
                through = dot(r.enter[rs.stop - 16 : rs.stop, :], r.widen[:, cols])[15:, :]
                new = new + through * r.state[i, :, cols]
            r.state[i + 1, :, cols] = new
            if i == chunks - 1:
                spans = [slice(c, c + LANES) for c in range(cols.start, cols.stop, LANES)]
                for span in spans:
                    r.leaving[span.start // LANES] = r.state[chunks, :, span].astype(BF16)

                @pl.when((pos == 0) & (pos < chain - 1))
                def _():
                    for span in spans:
                        down(span.start // LANES).start()

    def within(i):
        rs = chunk_rows(i)
        own_c = r.mapped[rs, NSTATE:]
        for cols in tiles:
            outer = dot(r.outer[rs, :], r.widen[:, cols])
            r.factor[rs, cols] = outer * r.gate[rs, cols]
            rest = r.skips[:1, cols] * r.inner[rs, cols].astype(F32)
            if i:
                carried = dot(own_c, r.state[i, :, cols].astype(BF16))
                rest = rest + dot(r.enter[rs, :], r.widen[:, cols]) * carried
            r.y[rs, cols] = rest
        for j in range(pairs):
            cols = slice(j * LANES, (j + 1) * LANES)
            x = r.inner[rs, cols]
            weights = []
            for h in range(per * j, per * (j + 1)):
                gap = r.cum[i, :, h : h + 1] - r.cumt[i, h : h + 1, :]
                weight = jnp.exp2(jnp.minimum(gap, 0.0)) * r.score[i] * r.stept[i, h : h + 1, :]
                weights.append(weight.astype(BF16))
            zero = jnp.zeros_like(x)
            split = jnp.concatenate([jnp.where(left, x, zero), jnp.where(left, zero, x)], axis=0)
            inside = dot(jnp.concatenate(weights, axis=1), split)
            r.y[rs, cols] = (r.y[rs, cols] + inside) * r.gate[rs, cols]

    r.before[...] = jnp.zeros_like(r.before)

    @pl.when(pos == 0)
    def _():
        r.arrived[...] = jnp.zeros_like(r.arrived)

    def relay(b):
        gathers[b][0].wait_recv()
        gathers[b][4].start()
        gathers[b][1].wait_recv()
        gathers[b][5].start()
        if b + 1 < blocks:
            for copy in gathers[b + 1][:4]:
                copy.start()

    def direct_here(b):
        gathers[b][2].wait_recv()
        gathers[b][3].wait_recv()

    def relayed_here(b):
        gathers[b][4].wait_recv()
        gathers[b][5].wait_recv()

    relay(0)
    for k in range(3):
        for copy in loads[k]:
            copy.wait()
    for b in range(blocks):
        final = b == blocks - 1
        direct_here(b)
        early(b, "x")
        early(b, "z")
        if b == 0:
            for copy in loads[3]:
                copy.wait()
            for copy in out_loads:
                copy.start()
        relayed_here(b)
        late_small(b)
        prepare(b)
        late_x(b)
        if not final:
            late_z(b)
        for i in range(b * parts, (b + 1) * parts):
            states(i)
        if final:
            late_z(b)
        for i in range(b * parts, (b + 1) * parts):
            within(i)
            if not final and i == b * parts:
                relay(b + 1)

    r.sums[...] = jnp.zeros_like(r.sums)

    def finish(c, _):
        cols = pl.ds(pl.multiple_of(c * LANES, LANES), LANES)

        @pl.when(pos > 0)
        def _():
            down(c).wait_recv()

            @pl.when(pos < chain - 1)
            def _():
                through = dot(r.outer[rows - 16 :, :], r.widen[:, cols])[15:, :]
                value = r.state[chunks, :, cols] + through * r.arrived[c].astype(F32)
                r.leaving[c] = value.astype(BF16)
                down(c).start()

        carried = dot(r.mapped[:, NSTATE:], r.arrived[c])
        gated = r.y[:, cols] + r.factor[:, cols] * carried
        r.g[:, cols] = (gated * r.gain[:, cols]).astype(BF16)
        r.sums[...] = r.sums[...] + gated * gated
        return 0

    lax.fori_loop(0, pairs, finish, 0)

    for copy in out_loads:
        copy.wait()
    small = [
        remote("head", to, r.squares.at[k], r.others.at[k], r.q_send.at[k], r.q_recv.at[k])
        for k, to in enumerate((across, along))
    ]
    scatters = [
        [
            remote("head", to, r.sent.at[6 * b + k], r.back.at[6 * b + k], r.o_send.at[6 * b + k], r.o_recv.at[6 * b + k])
            for k, to in enumerate((across, along, across, along, along, across))
        ]
        for b in range(blocks)
    ]

    def put(b, k, value):
        r.sent[6 * b + k] = value.astype(BF16)
        scatters[b][k].start()

    def share(k, rs):
        return dot(r.g[rs, :], r.vw[k])

    def direct(b):
        lo, hi = slice(b * GROUP, b * GROUP + half), slice(b * GROUP + half, (b + 1) * GROUP)
        put(b, 0, share(0, lo))
        put(b, 1, share(0, hi))
        put(b, 2, share(1, lo))
        put(b, 3, share(2, hi))

    def joined(b):
        lo, hi = slice(b * GROUP, b * GROUP + half), slice(b * GROUP + half, (b + 1) * GROUP)
        value = share(2, lo)
        scatters[b][0].wait_recv()
        put(b, 4, value + r.back[6 * b].astype(F32))
        value = share(1, hi)
        scatters[b][1].wait_recv()
        put(b, 5, value + r.back[6 * b + 1].astype(F32))

    slot = lax.broadcasted_iota(jnp.int32, (8, LANES), 0)
    for b in range(blocks):
        direct(b)
        if b == 0:
            squares = jnp.zeros((8, LANES), F32)
            for i in range(chunks):
                row = dot_nt(jnp.ones((8, LANES), F32), r.sums[chunk_rows(i), :], lax.Precision.HIGHEST)
                squares = jnp.where(slot == i, row, squares)
            r.squares[0] = squares
            small[0].start()
        if b:
            joined(b - 1)
    small[0].wait_recv()
    r.squares[1] = r.squares[0] + r.others[0]
    small[1].start()
    joined(blocks - 1)
    own = r.y
    for b in range(blocks):
        own[rows_of(b), :depth] = share(3, rows_of(b))
    small[1].wait_recv()
    scale = lax.rsqrt((r.squares[1] + r.others[1]) / total + EPS)
    for i in range(chunks):
        r.sums[chunk_rows(i), :] = jnp.broadcast_to(scale[i : i + 1, :], (LANES, CHUNK)).T
    stores = []
    for b in range(blocks):
        for base, picks in ((b * GROUP, (2, 4)), (b * GROUP + half, (3, 5))):
            span = slice(base, base + half)
            for k in picks:
                scatters[b][k].wait_recv()
            for i in range(depth // LANES):
                cols = slice(i * LANES, (i + 1) * LANES)
                value = own[span, cols]
                for k in picks:
                    value = value + r.back[6 * b + k, :, cols].astype(F32)
                r.result[span, cols] = (value * r.sums[span, :]).astype(BF16)
            stores.append(pltpu.make_async_copy(r.result.at[span], out.at[span], r.store.at[len(stores)]))
            stores[-1].start()

    for group in gathers + scatters + [small]:
        for copy in group:
            copy.wait_send()

    @pl.when(pos < chain - 1)
    def _():
        for c in range(pairs):
            down(c).wait_send()

    for copy in stores:
        copy.wait()


def layer(chain, split, tokens, resets, w_x, w_z, w_bc, w_dt, dt_bias, decay_rate, d_skip, norm_gain, w_out):
    rows, depth = tokens.shape
    width, heads, both = w_x.shape[1], w_dt.shape[1], w_bc.shape[1]
    blocks, pairs = rows // GROUP, width // LANES
    chunks = rows // CHUNK
    half = GROUP // 2
    vm, dma = pltpu.VMEM, pltpu.SemaphoreType.DMA
    scratch = dict(
        xt=vm((rows, 4 * depth), BF16),
        vx=vm((4 * depth, width), BF16),
        vz=vm((4 * depth, width), BF16),
        vb=vm((4 * depth, both), BF16),
        vw=vm((4, width, depth), BF16),
        wd=vm((LANES, 4 * depth), BF16),
        w_dt=vm((heads, 4 * depth), BF16),
        resets=vm((1, rows), jnp.int32),
        bias0=vm((1, heads), F32),
        rate0=vm((1, heads), F32),
        skip0=vm((1, heads), F32),
        bias=vm((1, LANES), F32),
        rate=vm((1, LANES), F32),
        skip=vm((1, LANES), F32),
        skips=vm((8, width), F32),
        gain=vm((1, width), F32),
        tri=vm((CHUNK, 3 * CHUNK), BF16),
        widen=vm((2 * LANES, width), BF16),
        mask=vm((chunks, CHUNK, CHUNK), F32),
        alone=vm((rows, LANES), F32),
        same=vm((rows, LANES), F32),
        open=vm((rows, LANES), F32),
        acc_x=vm((GROUP, width), F32),
        acc_z=vm((GROUP, width), F32),
        acc_m=vm((GROUP, both), F32),
        acc_s=vm((GROUP, LANES), F32),
        inner=vm((rows, width), BF16),
        gate=vm((rows, width), F32),
        mapped=vm((rows, both), BF16),
        turned=vm((chunks, NSTATE, CHUNK), BF16),
        step=vm((GROUP, LANES), F32),
        before=vm((chunks + 1, LANES), F32),
        cum=vm((chunks, CHUNK, LANES), F32),
        cumt=vm((chunks, LANES, CHUNK), F32),
        stept=vm((chunks, LANES, CHUNK), F32),
        keep=vm((rows, 2 * LANES), BF16),
        enter=vm((rows, 2 * LANES), BF16),
        outer=vm((rows, 2 * LANES), BF16),
        score=vm((chunks, CHUNK, CHUNK), F32),
        state=vm((chunks + 1, NSTATE, width), F32),
        arrived=vm((pairs, NSTATE, LANES), BF16),
        leaving=vm((pairs, NSTATE, LANES), BF16),
        y=vm((rows, width), F32),
        factor=vm((rows, width), F32),
        g=vm((rows, width), BF16),
        sums=vm((rows, LANES), F32),
        squares=vm((2, 8, LANES), F32),
        others=vm((2, 8, LANES), F32),
        sent=vm((6 * blocks, half, depth), BF16),
        back=vm((6 * blocks, half, depth), BF16),
        result=vm((rows, depth), BF16),
        small_load=dma((7,)),
        load=dma((12,)),
        load_out=dma((4,)),
        g_send=dma((6 * blocks,)),
        g_recv=dma((6 * blocks,)),
        c_send=dma((pairs,)),
        c_recv=dma((pairs,)),
        o_send=dma((6 * blocks,)),
        o_recv=dma((6 * blocks,)),
        q_send=dma((2,)),
        q_recv=dma((2,)),
        store=dma((2 * blocks,)),
    )
    return pl.pallas_call(
        functools.partial(kernel, chain, float(width * split), tuple(scratch)),
        out_shape=jax.ShapeDtypeStruct((rows, depth), BF16),
        in_specs=[ANY] * 11,
        out_specs=ANY,
        scratch_shapes=list(scratch.values()),
        compiler_params=pltpu.CompilerParams(
            collective_id=0, has_side_effects=True, vmem_limit_bytes=60 * 1024 * 1024
        ),
    )(
        tokens, resets.reshape(1, rows), w_x, w_z, w_bc, w_dt.T, dt_bias.reshape(1, heads),
        decay_rate.reshape(1, heads), d_skip.reshape(1, heads), norm_gain.reshape(1, width), w_out,
    )


def solution(mesh):
    in_specs = (
        P(("batch", "seq"), "head"),
        P(("batch", "seq")),
        P(None, "head"),
        P(None, "head"),
        P(),
        P(None, "head"),
        P("head"),
        P("head"),
        P("head"),
        P("head"),
        P("head", None),
    )
    return jax.shard_map(
        functools.partial(layer, mesh.shape["seq"], mesh.shape["head"]),
        mesh=mesh,
        in_specs=in_specs,
        out_specs=P(("batch", "seq"), "head"),
        check_vma=False,
    )
```

```python
import functools
import math

import jax
import jax.numpy as jnp
from jax import lax
from jax.experimental import pallas as pl
from jax.experimental.pallas import tpu as pltpu
from jax.sharding import PartitionSpec as P

HEADDIM = 64
NSTATE = 128
GROUP = 256
LANES = 128
CHUNK = 128
WIDE = 256
F32 = jnp.float32
BF16 = jnp.bfloat16
MESH = pl.DeviceIdType.MESH
ANY = pl.BlockSpec(memory_space=pl.ANY)
EPS = 1e-05
LOG2E = math.log2(math.e)


def peers():
    me = lax.axis_index("head")
    across = me + 1 - 2 * lax.rem(me, 2)
    along = lax.rem(me + 2, 4)
    corner = lax.rem(across + 2, 4)
    return me, across, along, corner


def remote(axis, to, src, dst, send, recv):
    return pltpu.make_async_remote_copy(
        src_ref=src, dst_ref=dst, send_sem=send, recv_sem=recv, device_id={axis: to}, device_id_type=MESH
    )


def silu(v):
    return v / (1.0 + jnp.exp(-v))


class Scratch:
    def __init__(self, names, refs):
        for name, ref in zip(names, refs):
            setattr(self, name, ref)


def dot(a, b):
    return jnp.dot(a, b, preferred_element_type=F32)


def dot_nt(a, b, precision=None):
    return lax.dot_general(a, b, (((1,), (1,)), ((), ())), preferred_element_type=F32, precision=precision)


def two_terms(v):
    high = v.astype(BF16)
    return jnp.concatenate([high, (v - high.astype(F32)).astype(BF16)], axis=1)


def kernel(chain, cores, total, names, tok, resets, w_x, w_z, w_bc, w_dt, bias, rate, skip, gain, w_out, out, *refs):
    r = Scratch(names, refs)
    me, across, along, corner = peers()
    pos = lax.axis_index("seq")
    upper, lower = lax.rem(pos + 1, chain), lax.rem(pos + chain - 1, chain)
    rows, depth = tok.shape
    width = w_x.shape[1]
    heads = w_dt.shape[0]
    core, other_core = lax.axis_index("batch"), 1 - lax.axis_index("batch")
    blocks, pairs, per = rows // GROUP, width // LANES, LANES // HEADDIM
    half = GROUP // 2
    chunks, parts = rows // CHUNK, GROUP // CHUNK
    cuts = (0, depth // WIDE * WIDE, 3 * depth // WIDE * WIDE, 4 * depth)
    owners = (me, across, along, corner)
    tiles = [slice(i, min(i + WIDE, width)) for i in range(0, width, WIDE)]

    def span_of(owner):
        return pl.ds(pl.multiple_of(owner * depth, LANES), depth)

    def place(k):
        return slice(k * depth, (k + 1) * depth)

    def rows_of(b):
        return slice(b * GROUP, (b + 1) * GROUP)

    def chunk_rows(i):
        return slice(i * CHUNK, (i + 1) * CHUNK)

    own_tokens = pltpu.make_async_copy(tok, r.xt.at[:, place(0)], r.small_load.at[0])
    own_tokens.start()
    barrier = pltpu.get_barrier_semaphore()
    for other in (across, along):
        pl.semaphore_signal(barrier, inc=1, device_id={"head": other}, device_id_type=MESH)
    for other in (upper, lower):
        pl.semaphore_signal(barrier, inc=1, device_id={"seq": other}, device_id_type=MESH)
    if cores == 2:
        pl.semaphore_signal(barrier, inc=1, device_id={"batch": other_core}, device_id_type=MESH)
    smalls = [
        pltpu.make_async_copy(src, dst, r.small_load.at[1 + i])
        for i, (src, dst) in enumerate(
            (
                (resets, r.resets), (w_dt, r.w_dt), (bias, r.bias0), (rate, r.rate0), (skip, r.skip0), (gain, r.gain0),
            )
        )
    ]
    for copy in smalls:
        copy.start()
    loads = [
        (
            pltpu.make_async_copy(w_x.at[span_of(owner)], r.vx.at[place(k)], r.load.at[3 * k]),
            pltpu.make_async_copy(w_z.at[span_of(owner)], r.vz.at[place(k)], r.load.at[3 * k + 1]),
            pltpu.make_async_copy(w_bc.at[span_of(owner)], r.vb.at[place(k)], r.load.at[3 * k + 2]),
        )
        for k, owner in enumerate(owners)
    ]
    order = (corner, across, along, me)
    out_loads = [
        pltpu.make_async_copy(w_out.at[:, span_of(owner)], r.vw.at[k], r.load_out.at[k])
        for k, owner in enumerate(order)
    ]
    for group in loads:
        for copy in group:
            copy.start()

    gathers = []
    for b in range(blocks):
        lo = slice(b * GROUP, b * GROUP + half)
        hi = slice(b * GROUP + half, (b + 1) * GROUP)
        plan = (
            (across, r.xt.at[lo, place(0)], r.xt.at[lo, place(1)]),
            (along, r.xt.at[hi, place(0)], r.xt.at[hi, place(2)]),
            (across, r.xt.at[hi, place(0)], r.xt.at[hi, place(1)]),
            (along, r.xt.at[lo, place(0)], r.xt.at[lo, place(2)]),
            (along, r.xt.at[lo, place(1)], r.xt.at[lo, place(3)]),
            (across, r.xt.at[hi, place(2)], r.xt.at[hi, place(3)]),
        )
        gathers.append([
            remote("head", to, src, dst, r.g_send.at[6 * b + i], r.g_recv.at[6 * b + i])
            for i, (to, src, dst) in enumerate(plan)
        ])
    own_tokens.wait()
    pl.semaphore_wait(barrier, 4 + cores // 2)

    def send_first():
        for copy in gathers[0][:4]:
            copy.start()
        for copies in gathers[1:]:
            for copy in copies[:2]:
                copy.start()

    @pl.when(core == 0)
    def _():
        send_first()

    ti = lax.broadcasted_iota(jnp.int32, (CHUNK, CHUNK), 0)
    si = lax.broadcasted_iota(jnp.int32, (CHUNK, CHUNK), 1)
    causal = ti >= si
    tri = jnp.where(causal, 1.0, 0.0).astype(F32)
    left = si < HEADDIM
    for k in range(3):
        r.tri[:, k * CHUNK : (k + 1) * CHUNK] = tri.astype(BF16)
    for cols in tiles:
        shape = (2 * LANES, cols.stop - cols.start)
        channel = lax.broadcasted_iota(jnp.int32, shape, 1) + cols.start
        source = lax.rem(lax.broadcasted_iota(jnp.int32, shape, 0), LANES)
        inside = (channel >= source * HEADDIM) & (channel < (source + 1) * HEADDIM)
        r.widen[:, cols] = jnp.where(inside, 1.0, 0.0).astype(BF16)
    for copy in smalls:
        copy.wait()
    r.rate[...] = jnp.zeros_like(r.rate)
    r.rate[:, :heads] = r.rate0[...] * LOG2E
    r.bias[...] = jnp.zeros_like(r.bias)
    r.bias[:, :heads] = r.bias0[...]
    r.skip[...] = jnp.zeros_like(r.skip)
    r.skip[:, :heads] = r.skip0[...]
    r.wd[...] = jnp.zeros_like(r.wd)
    for k, owner in enumerate(owners):
        r.wd[:heads, place(k)] = r.w_dt[:, span_of(owner)]
    for j in range(pairs):
        r.gain[:, j * LANES : (j + 1) * LANES] = r.gain0[j : j + 1, :]
    spare = jnp.broadcast_to(r.skip[...], (8, LANES))
    for cols in tiles:
        r.skips[:, cols] = dot(two_terms(spare), r.widen[:, cols])
    seen = jnp.zeros((1, LANES), F32)
    for i in range(chunks):
        rs = chunk_rows(i)
        starts = r.resets[:, rs].astype(F32)
        seg = jnp.broadcast_to(jnp.sum(tri * starts, axis=1, keepdims=True), (CHUNK, CHUNK))
        last = seg[CHUNK - 1 :, :]
        r.mask[i] = jnp.where(causal & (seg == seg.T), 1.0, 0.0)
        r.alone[rs, :] = jnp.where(seg == 0.0, 1.0, 0.0)
        r.same[rs, :] = jnp.where(seg == last, 1.0, 0.0)
        r.open[rs, :] = jnp.where(seg + seen == 0.0, 1.0, 0.0)
        seen = seen + last

    def projected(b, k, what):
        rs, span = rows_of(b), slice(cuts[k], cuts[k + 1])

        def add(acc, cols, value):
            acc[rs, cols] = value if k == 0 else acc[rs, cols] + value

        if "x" in what:
            add(r.acc_m, slice(None), dot(r.xt[rs, span], r.vb[span, :]))
            add(r.acc_s, slice(None), dot_nt(r.xt[rs, span], r.wd[:, span]))
            for cols in tiles:
                add(r.acc_x, cols, dot(r.xt[rs, span], r.vx[span, cols]))
        if "z" in what:
            for cols in tiles:
                add(r.acc_z, cols, dot(r.xt[rs, span], r.vz[span, cols]))

    def late_small(b):
        rs, span = rows_of(b), slice(cuts[2], cuts[3])
        x = r.xt.at[rs, span]
        r.mapped[rs, :] = silu(r.acc_m[rs, :] + dot(x[...], r.vb[span, :])).astype(BF16)
        v = r.acc_s[rs, :] + dot_nt(x[...], r.wd[:, span]) + r.bias[...]
        r.step[...] = jnp.maximum(v, 0.0) + jnp.log1p(jnp.exp(-jnp.abs(v)))

    def late_x(b, cols):
        rs, span = rows_of(b), slice(cuts[2], cuts[3])
        r.inner[rs, cols] = silu(r.acc_x[rs, cols] + dot(r.xt[rs, span], r.vx[span, cols])).astype(BF16)

    def late_z(b):
        rs, span = rows_of(b), slice(cuts[2], cuts[3])
        for cols in tiles:
            z = (r.acc_z[rs, cols] + dot(r.xt[rs, span], r.vz[span, cols])).astype(BF16).astype(F32)
            r.gate[rs, cols] = silu(z)

    def prepare(b):
        leaves, through = [], None
        for i in range(b * parts, (b + 1) * parts):
            rs = chunk_rows(i)
            stp = r.step[(i - b * parts) * CHUNK : (i - b * parts + 1) * CHUNK, :]
            decay = -stp * r.rate[...]
            high = decay.astype(BF16)
            rest = decay - high.astype(F32)
            middle = rest.astype(BF16)
            low = (rest - middle.astype(F32)).astype(BF16)
            cum = dot(r.tri[...], jnp.concatenate([high, middle, low], axis=0))
            last = cum[CHUNK - 1 :, :]
            before = r.before[i : i + 1, :]
            r.before[i + 1 : i + 2, :] = before + last
            r.cum[i] = cum
            r.cumt[i] = cum.T
            r.stept[i] = stp.T
            keep = r.same[rs, :] * jnp.exp2(last - cum) * stp
            r.keep[rs, :] = two_terms(keep)
            enter = r.alone[rs, :] * jnp.exp2(cum)
            outer = r.open[rs, :] * jnp.exp2(before + cum)
            r.enter[rs, :] = two_terms(enter)
            r.outer[rs, :] = two_terms(outer)
            passed = enter[CHUNK - 1 :, :]
            leaves = [value * passed for value in leaves] + [keep]
            through = passed if through is None else through * passed
            mapped_b, mapped_c = r.mapped[rs, :NSTATE], r.mapped[rs, NSTATE:]
            r.score[i] = r.mask[i] * dot_nt(mapped_c, mapped_b)
            turned = mapped_b.astype(F32).T.astype(BF16)
            r.turned[b, :, (i - b * parts) * CHUNK : (i - b * parts + 1) * CHUNK] = turned
        r.leave[...] = two_terms(jnp.concatenate(leaves, axis=0))
        slot = lax.broadcasted_iota(jnp.int32, (8, LANES), 0)
        ends = jnp.where(slot == 0, through, outer[CHUNK - 1 :, :])
        r.ends[...] = two_terms(ends)

    def down(c):
        return remote("seq", upper, r.leaving.at[c], r.arrived.at[c], r.c_send.at[c], r.c_recv.at[c])

    def widened(ref, rs, cols):
        return dot(ref[rs, :], r.widen[:, cols])

    def block_state(b, cols):
        rs = rows_of(b)
        scaled = (dot(r.leave[...], r.widen[:, cols]) * r.inner[rs, cols].astype(F32)).astype(BF16)
        new = dot(r.turned[b], scaled)
        if b:
            ends = dot(r.ends[...], r.widen[:, cols])
            r.through[:, cols] = ends
            new = new + ends[:1, :] * r.state[b - 1, :, cols]
        r.state[b, :, cols] = new

    def departures(cols):
        return range(cols.start // LANES, cols.stop // LANES)

    def leave_first(cols):
        for c in departures(cols):
            r.leaving[c] = r.state[blocks - 1, :, c * LANES : (c + 1) * LANES].astype(BF16)

        @pl.when((pos == 0) & (pos < chain - 1))
        def _():
            for c in departures(cols):
                down(c).start()

    def pass_on(c, cols):
        value = r.state[blocks - 1, :, cols] + r.through[1:2, cols] * r.arrived[c].astype(F32)
        r.leaving[c] = value.astype(BF16)
        down(c).start()

    def slot(at, picks):
        if picks and chain > at + 1:

            @pl.when(pos == at)
            def _():
                for c in picks:
                    down(c).wait_recv()
                    pass_on(c, slice(c * LANES, (c + 1) * LANES))

    def middle(i):
        b = i // parts
        rs = chunk_rows(i - 1)
        turned = r.turned[b, :, (i - 1 - b * parts) * CHUNK : (i - b * parts) * CHUNK]
        for cols in tiles:
            scaled = (widened(r.keep, rs, cols) * r.inner[rs, cols].astype(F32)).astype(BF16)
            new = dot(turned, scaled)
            if i > 1:
                passed = dot(r.enter[rs.stop - 16 : rs.stop, :], r.widen[:, cols])[15:, :]
                new = new + passed * (r.mid[...][:, cols] if (i - 1) % parts else r.state[b - 1, :, cols])
            r.mid[:, cols] = new

    def within(i):
        rs = chunk_rows(i)
        own_c = r.mapped[rs, NSTATE:]
        for cols in tiles:
            outer = dot(r.outer[rs, :], r.widen[:, cols])
            r.factor[rs, cols] = outer * r.gate[rs, cols]
            rest = r.skips[:1, cols] * r.inner[rs, cols].astype(F32)
            if i:
                start = r.mid[:, cols] if i % parts else r.state[i // parts - 1, :, cols]
                carried = dot(own_c, start.astype(BF16))
                rest = rest + dot(r.enter[rs, :], r.widen[:, cols]) * carried
            r.y[rs, cols] = rest
        for j in range(pairs):
            cols = slice(j * LANES, (j + 1) * LANES)
            x = r.inner[rs, cols]
            weights = []
            for h in range(per * j, per * (j + 1)):
                gap = r.cum[i, :, h : h + 1] - r.cumt[i, h : h + 1, :]
                weight = jnp.exp2(jnp.minimum(gap, 0.0)) * r.score[i] * r.stept[i, h : h + 1, :]
                weights.append(weight.astype(BF16))
            zero = jnp.zeros_like(x)
            split = jnp.concatenate([jnp.where(left, x, zero), jnp.where(left, zero, x)], axis=0)
            inside = dot(jnp.concatenate(weights, axis=1), split)
            r.y[rs, cols] = (r.y[rs, cols] + inside) * r.gate[rs, cols]

    r.before[...] = jnp.zeros_like(r.before)

    @pl.when(pos == 0)
    def _():
        r.arrived[...] = jnp.zeros_like(r.arrived)

    def relay(b):
        gathers[b][0].wait_recv()
        gathers[b][4].start()
        gathers[b][1].wait_recv()
        gathers[b][5].start()
        if b + 1 < blocks:
            for copy in gathers[b + 1][2:4]:
                copy.start()

    def direct_here(b):
        gathers[b][2].wait_recv()
        gathers[b][3].wait_recv()

    def relayed_here(b):
        gathers[b][4].wait_recv()
        gathers[b][5].wait_recv()

    for copy in loads[0]:
        copy.wait()
    for b in range(blocks):
        projected(b, 0, "xz")
    if cores == 2:

        @pl.when(core == 1)
        def _():
            pl.semaphore_wait(r.go.at[0], 1)
            send_first()

    relay(0)
    for k in (1, 2):
        for copy in loads[k]:
            copy.wait()
    for b in range(blocks):
        direct_here(b)
        projected(b, 1, "x")
        if b == 0:
            projected(b, 1, "z")
            for copy in loads[3]:
                copy.wait()
            for copy in out_loads:
                copy.start()
        if b + 1 < blocks:
            relay(b + 1)
        relayed_here(b)
        late_small(b)
        prepare(b)
        if b == 0 and cores == 2:

            @pl.when(core == 0)
            def _():
                pl.semaphore_signal(r.go.at[0], inc=1, device_id={"batch": other_core}, device_id_type=MESH)

        if b + 1 < blocks:
            for cols in tiles:
                late_x(b, cols)
            for cols in tiles:
                block_state(b, cols)
        else:
            late_x(b, tiles[0])
            for k, cols in enumerate(tiles):
                if k + 1 < len(tiles):
                    late_x(b, tiles[k + 1])
                block_state(b, cols)
                leave_first(cols)

    picks = [range(pairs * k // 10, pairs * (k + 1) // 10) for k in range(10)]

    def picked(low, high):
        return [c for k in range(low, high) for c in picks[k]]

    late_count = pairs * 8 // 10
    late_z(0)
    for b in range(1, blocks):
        projected(b, 1, "z")
    slot(1, picked(0, 1))
    for b in range(1, blocks):
        late_z(b)
    slot(1, picked(1, 4))
    passes = {0: ((4, 6), (0, 0)), 1: ((6, 10), (0, 2)), 2: ((0, 0), (2, 5)), 3: ((0, 0), (5, 8))}
    for i in range(chunks):
        if i % parts:
            middle(i)
        within(i)
        for at in (1, 2):
            slot(at, picked(*passes[i][at - 1]))

    r.sums[...] = jnp.zeros_like(r.sums)

    def finish(c, _):
        cols = pl.ds(pl.multiple_of(c * LANES, LANES), LANES)

        @pl.when((pos > 2) | ((pos == 2) & (c >= late_count)) | ((pos > 0) & (pos == chain - 1)))
        def _():
            down(c).wait_recv()

            @pl.when(pos < chain - 1)
            def _():
                pass_on(c, cols)

        carried = dot(r.mapped[:, NSTATE:], r.arrived[c])
        gated = r.y[:, cols] + r.factor[:, cols] * carried
        r.g[:, cols] = (gated * r.gain[:, cols]).astype(BF16)
        r.sums[...] = r.sums[...] + gated * gated
        return 0

    lax.fori_loop(0, pairs, finish, 0)

    for copy in out_loads:
        copy.wait()
    small = [
        remote("head", to, r.squares.at[k], r.others.at[k], r.q_send.at[k], r.q_recv.at[k])
        for k, to in enumerate((across, along))
    ]
    scatters = [
        [
            remote("head", to, r.sent.at[6 * b + k], r.back.at[6 * b + k], r.o_send.at[6 * b + k], r.o_recv.at[6 * b + k])
            for k, to in enumerate((across, along, across, along, along, across))
        ]
        for b in range(blocks)
    ]

    def put(b, k, value):
        r.sent[6 * b + k] = value.astype(BF16)
        scatters[b][k].start()

    def share(k, rs):
        return dot(r.g[rs, :], r.vw[k])

    def direct(b):
        lo, hi = slice(b * GROUP, b * GROUP + half), slice(b * GROUP + half, (b + 1) * GROUP)
        put(b, 0, share(0, lo))
        put(b, 1, share(0, hi))
        put(b, 2, share(1, lo))
        put(b, 3, share(2, hi))

    def joined(b):
        lo, hi = slice(b * GROUP, b * GROUP + half), slice(b * GROUP + half, (b + 1) * GROUP)
        value = share(2, lo)
        scatters[b][0].wait_recv()
        put(b, 4, value + r.back[6 * b].astype(F32))
        value = share(1, hi)
        scatters[b][1].wait_recv()
        put(b, 5, value + r.back[6 * b + 1].astype(F32))

    slot = lax.broadcasted_iota(jnp.int32, (8, LANES), 0)
    for b in range(blocks):
        direct(b)
        if b == 0:
            squares = jnp.zeros((8, LANES), F32)
            for i in range(chunks):
                row = dot_nt(jnp.ones((8, LANES), F32), r.sums[chunk_rows(i), :], lax.Precision.HIGHEST)
                squares = jnp.where(slot == i, row, squares)
            r.squares[0] = squares
            small[0].start()
        if b:
            joined(b - 1)
    small[0].wait_recv()
    r.squares[1] = r.squares[0] + r.others[0]
    small[1].start()
    joined(blocks - 1)
    own = r.y
    for b in range(blocks):
        own[rows_of(b), :depth] = share(3, rows_of(b))
    small[1].wait_recv()
    scale = lax.rsqrt((r.squares[1] + r.others[1]) / total + EPS)
    for i in range(chunks):
        r.sums[chunk_rows(i), :] = jnp.broadcast_to(scale[i : i + 1, :], (LANES, CHUNK)).T
    for b in range(blocks):
        for base, picks in ((b * GROUP, (2, 4)), (b * GROUP + half, (3, 5))):
            span = slice(base, base + half)
            for k in picks:
                scatters[b][k].wait_recv()
            for i in range(depth // LANES):
                cols = slice(i * LANES, (i + 1) * LANES)
                value = own[span, cols]
                for k in picks:
                    value = value + r.back[6 * b + k, :, cols].astype(F32)
                out[span, cols] = (value * r.sums[span, :]).astype(BF16)

    for group in gathers + scatters + [small]:
        for copy in group:
            copy.wait_send()

    @pl.when(pos < chain - 1)
    def _():
        for c in range(pairs):
            down(c).wait_send()


def layer(chain, split, cores, tokens, resets, w_x, w_z, w_bc, w_dt, dt_bias, decay_rate, d_skip, norm_gain, w_out):
    rows, depth = tokens.shape
    width, heads, both = w_x.shape[1], w_dt.shape[1], w_bc.shape[1]
    blocks, pairs = rows // GROUP, width // LANES
    chunks = rows // CHUNK
    half = GROUP // 2
    vm, dma = pltpu.VMEM, pltpu.SemaphoreType.DMA
    scratch = dict(
        xt=vm((rows, 4 * depth), BF16),
        vx=vm((4 * depth, width), BF16),
        vz=vm((4 * depth, width), BF16),
        vb=vm((4 * depth, both), BF16),
        vw=vm((4, width, depth), BF16),
        wd=vm((LANES, 4 * depth), BF16),
        w_dt=vm((heads, 4 * depth), BF16),
        resets=vm((1, rows), jnp.int32),
        bias0=vm((1, heads), F32),
        rate0=vm((1, heads), F32),
        skip0=vm((1, heads), F32),
        bias=vm((1, LANES), F32),
        rate=vm((1, LANES), F32),
        skip=vm((1, LANES), F32),
        skips=vm((8, width), F32),
        gain0=vm((pairs, LANES), F32),
        gain=vm((1, width), F32),
        tri=vm((CHUNK, 3 * CHUNK), BF16),
        widen=vm((2 * LANES, width), BF16),
        mask=vm((chunks, CHUNK, CHUNK), F32),
        alone=vm((rows, LANES), F32),
        same=vm((rows, LANES), F32),
        open=vm((rows, LANES), F32),
        acc_x=vm((rows, width), F32),
        acc_z=vm((rows, width), F32),
        acc_m=vm((rows, both), F32),
        acc_s=vm((rows, LANES), F32),
        inner=vm((rows, width), BF16),
        gate=vm((rows, width), F32),
        mapped=vm((rows, both), BF16),
        turned=vm((blocks, NSTATE, GROUP), BF16),
        leave=vm((GROUP, 2 * LANES), BF16),
        ends=vm((8, 2 * LANES), BF16),
        through=vm((8, width), F32),
        mid=vm((NSTATE, width), F32),
        step=vm((GROUP, LANES), F32),
        before=vm((chunks + 1, LANES), F32),
        cum=vm((chunks, CHUNK, LANES), F32),
        cumt=vm((chunks, LANES, CHUNK), F32),
        stept=vm((chunks, LANES, CHUNK), F32),
        keep=vm((rows, 2 * LANES), BF16),
        enter=vm((rows, 2 * LANES), BF16),
        outer=vm((rows, 2 * LANES), BF16),
        score=vm((chunks, CHUNK, CHUNK), F32),
        state=vm((blocks, NSTATE, width), F32),
        arrived=vm((pairs, NSTATE, LANES), BF16),
        leaving=vm((pairs, NSTATE, LANES), BF16),
        y=vm((rows, width), F32),
        factor=vm((rows, width), F32),
        g=vm((rows, width), BF16),
        sums=vm((rows, LANES), F32),
        squares=vm((2, 8, LANES), F32),
        others=vm((2, 8, LANES), F32),
        sent=vm((6 * blocks, half, depth), BF16),
        back=vm((6 * blocks, half, depth), BF16),
        small_load=dma((7,)),
        load=dma((12,)),
        load_out=dma((4,)),
        g_send=dma((6 * blocks,)),
        g_recv=dma((6 * blocks,)),
        c_send=dma((pairs,)),
        c_recv=dma((pairs,)),
        o_send=dma((6 * blocks,)),
        o_recv=dma((6 * blocks,)),
        q_send=dma((2,)),
        q_recv=dma((2,)),
        go=pltpu.SemaphoreType.REGULAR((1,)),
    )
    return pl.pallas_call(
        functools.partial(kernel, chain, cores, float(width * split), tuple(scratch)),
        out_shape=pltpu.VMEM((rows, depth), BF16),
        in_specs=[ANY] * 11,
        out_specs=pl.BlockSpec(memory_space=pltpu.VMEM),
        scratch_shapes=list(scratch.values()),
        compiler_params=pltpu.CompilerParams(
            collective_id=0, has_side_effects=True, vmem_limit_bytes=60 * 1024 * 1024
        ),
    )(
        tokens, resets.reshape(1, rows), w_x, w_z, w_bc, w_dt.T, dt_bias.reshape(1, heads),
        decay_rate.reshape(1, heads), d_skip.reshape(1, heads), norm_gain.reshape(pairs, LANES), w_out,
    )


def solution(mesh):
    in_specs = (
        P(("batch", "seq"), "head"),
        P(("batch", "seq")),
        P(None, "head"),
        P(None, "head"),
        P(),
        P(None, "head"),
        P("head"),
        P("head"),
        P("head"),
        P("head"),
        P("head", None),
    )
    return jax.shard_map(
        functools.partial(layer, mesh.shape["seq"], mesh.shape["head"], mesh.shape["batch"]),
        mesh=mesh,
        in_specs=in_specs,
        out_specs=P(("batch", "seq"), "head"),
        check_vma=False,
    )
```

```python
import functools
import math

import jax
import jax.numpy as jnp
from jax import lax
from jax.experimental import pallas as pl
from jax.experimental.pallas import tpu as pltpu
from jax.sharding import PartitionSpec as P

HEADDIM = 64
NSTATE = 128
GROUP = 256
LANES = 128
CHUNK = 128
WIDE = 256
F32 = jnp.float32
BF16 = jnp.bfloat16
MESH = pl.DeviceIdType.MESH
ANY = pl.BlockSpec(memory_space=pl.ANY)
EPS = 1e-05
LOG2E = math.log2(math.e)


def peers():
    me = lax.axis_index("head")
    across = me + 1 - 2 * lax.rem(me, 2)
    along = lax.rem(me + 2, 4)
    corner = lax.rem(across + 2, 4)
    return me, across, along, corner


def remote(axis, to, src, dst, send, recv):
    return pltpu.make_async_remote_copy(
        src_ref=src, dst_ref=dst, send_sem=send, recv_sem=recv, device_id={axis: to}, device_id_type=MESH
    )


def silu(v):
    return v / (1.0 + jnp.exp(-v))


class Scratch:
    def __init__(self, names, refs):
        for name, ref in zip(names, refs):
            setattr(self, name, ref)


def dot(a, b):
    return jnp.dot(a, b, preferred_element_type=F32)


def dot_nt(a, b, precision=None):
    return lax.dot_general(a, b, (((1,), (1,)), ((), ())), preferred_element_type=F32, precision=precision)


def two_terms(v):
    high = v.astype(BF16)
    return jnp.concatenate([high, (v - high.astype(F32)).astype(BF16)], axis=1)


def kernel(chain, cores, total, names, tok, resets, w_x, w_z, w_bc, w_dt, bias, rate, skip, gain, w_out, out, *refs):
    r = Scratch(names, refs)
    me, across, along, corner = peers()
    pos = lax.axis_index("seq")
    upper, lower = lax.rem(pos + 1, chain), lax.rem(pos + chain - 1, chain)
    rows, depth = tok.shape
    width = w_x.shape[1]
    heads = w_dt.shape[0]
    core, other_core = lax.axis_index("batch"), 1 - lax.axis_index("batch")
    blocks, pairs, per = rows // GROUP, width // LANES, LANES // HEADDIM
    half = GROUP // 2
    chunks, parts = rows // CHUNK, GROUP // CHUNK
    cuts = (0, depth // WIDE * WIDE, 3 * depth // WIDE * WIDE, 4 * depth)
    owners = (me, across, along, corner)
    tiles = [slice(i, min(i + WIDE, width)) for i in range(0, width, WIDE)]

    def span_of(owner):
        return pl.ds(pl.multiple_of(owner * depth, LANES), depth)

    def place(k):
        return slice(k * depth, (k + 1) * depth)

    def rows_of(b):
        return slice(b * GROUP, (b + 1) * GROUP)

    def chunk_rows(i):
        return slice(i * CHUNK, (i + 1) * CHUNK)

    own_tokens = pltpu.make_async_copy(tok, r.xt.at[:, place(0)], r.small_load.at[0])
    own_tokens.start()
    barrier = pltpu.get_barrier_semaphore()
    for other in (across, along):
        pl.semaphore_signal(barrier, inc=1, device_id={"head": other}, device_id_type=MESH)

    @pl.when(pos > 0)
    def _():
        pl.semaphore_signal(barrier, inc=1, device_id={"seq": lower}, device_id_type=MESH)

    if cores == 2:
        pl.semaphore_signal(barrier, inc=1, device_id={"batch": other_core}, device_id_type=MESH)
    smalls = [
        pltpu.make_async_copy(src, dst, r.small_load.at[1 + i])
        for i, (src, dst) in enumerate(
            (
                (resets, r.resets), (w_dt, r.w_dt), (bias, r.bias0), (rate, r.rate0), (skip, r.skip0), (gain, r.gain0),
            )
        )
    ]
    for copy in smalls:
        copy.start()
    loads = [
        (
            pltpu.make_async_copy(w_x.at[span_of(owner)], r.vx.at[place(k)], r.load.at[3 * (k % 3)]),
            pltpu.make_async_copy(w_z.at[span_of(owner)], r.vz.at[place(k)], r.load.at[3 * (k % 3) + 1]),
            pltpu.make_async_copy(w_bc.at[span_of(owner)], r.vb.at[place(k)], r.load.at[3 * (k % 3) + 2]),
        )
        for k, owner in enumerate(owners)
    ]
    order = (corner, across, along, me)
    out_loads = [
        pltpu.make_async_copy(w_out.at[:, span_of(owner)], r.vw.at[k], r.load.at[3 + k])
        for k, owner in enumerate(order)
    ]
    for group in loads[:3]:
        for copy in group:
            copy.start()

    gathers = []
    for b in range(blocks):
        lo = slice(b * GROUP, b * GROUP + half)
        hi = slice(b * GROUP + half, (b + 1) * GROUP)
        plan = (
            (across, r.xt.at[lo, place(0)], r.xt.at[lo, place(1)]),
            (along, r.xt.at[hi, place(0)], r.xt.at[hi, place(2)]),
            (across, r.xt.at[hi, place(0)], r.xt.at[hi, place(1)]),
            (along, r.xt.at[lo, place(0)], r.xt.at[lo, place(2)]),
            (along, r.xt.at[lo, place(1)], r.xt.at[lo, place(3)]),
            (across, r.xt.at[hi, place(2)], r.xt.at[hi, place(3)]),
        )
        gathers.append([
            remote("head", to, src, dst, r.g_send.at[0], r.g_recv.at[4 * b + min(i, 2) + i // 4])
            for i, (to, src, dst) in enumerate(plan)
        ])
    own_tokens.wait()

    @pl.when(pos < chain - 1)
    def _():
        pl.semaphore_wait(barrier, 3 + cores // 2)

    @pl.when(pos == chain - 1)
    def _():
        pl.semaphore_wait(barrier, 2 + cores // 2)


    def send_first():
        for copy in gathers[0][:4]:
            copy.start()
        for copies in gathers[1:]:
            for copy in copies[:2]:
                copy.start()

    @pl.when(core == 0)
    def _():
        send_first()

    ti = lax.broadcasted_iota(jnp.int32, (CHUNK, CHUNK), 0)
    si = lax.broadcasted_iota(jnp.int32, (CHUNK, CHUNK), 1)
    causal = ti >= si
    tri = jnp.where(causal, 1.0, 0.0).astype(F32)
    left = si < HEADDIM
    for k in range(3):
        r.tri[:, k * CHUNK : (k + 1) * CHUNK] = tri.astype(BF16)
    for cols in tiles:
        shape = (2 * LANES, cols.stop - cols.start)
        channel = lax.broadcasted_iota(jnp.int32, shape, 1) + cols.start
        source = lax.rem(lax.broadcasted_iota(jnp.int32, shape, 0), LANES)
        inside = (channel >= source * HEADDIM) & (channel < (source + 1) * HEADDIM)
        r.widen[:, cols] = jnp.where(inside, 1.0, 0.0).astype(BF16)
    for copy in smalls:
        copy.wait()
    r.rate[...] = jnp.zeros_like(r.rate)
    r.rate[:, :heads] = r.rate0[...] * LOG2E
    r.bias[...] = jnp.zeros_like(r.bias)
    r.bias[:, :heads] = r.bias0[...]
    r.skip[...] = jnp.zeros_like(r.skip)
    r.skip[:, :heads] = r.skip0[...]
    r.wd[...] = jnp.zeros_like(r.wd)
    for k, owner in enumerate(owners):
        r.wd[:heads, place(k)] = r.w_dt[:, span_of(owner)]
    for j in range(pairs):
        r.gain[:, j * LANES : (j + 1) * LANES] = r.gain0[j : j + 1, :]
    spare = jnp.broadcast_to(r.skip[...], (8, LANES))
    for cols in tiles:
        r.skips[:, cols] = dot(two_terms(spare), r.widen[:, cols])
    seen = jnp.zeros((1, LANES), F32)
    for i in range(chunks):
        rs = chunk_rows(i)
        starts = r.resets[:, rs].astype(F32)
        seg = jnp.broadcast_to(jnp.sum(tri * starts, axis=1, keepdims=True), (CHUNK, CHUNK))
        last = seg[CHUNK - 1 :, :]
        r.mask[i] = jnp.where(causal & (seg == seg.T), 1.0, 0.0)
        r.alone[rs, :] = jnp.where(seg == 0.0, 1.0, 0.0)
        r.same[rs, :] = jnp.where(seg == last, 1.0, 0.0)
        r.open[rs, :] = jnp.where(seg + seen == 0.0, 1.0, 0.0)
        seen = seen + last

    some = len(tiles) // 2

    def projected(b, k, what, part=None):
        rs, span = rows_of(b), slice(cuts[k], cuts[k + 1])

        def add(acc, cols, value):
            acc[rs, cols] = value if k == 0 else acc[rs, cols] + value

        if "x" in what:
            add(r.acc_m, slice(None), dot(r.xt[rs, span], r.vb[span, :]))
            add(r.acc_s, slice(None), dot_nt(r.xt[rs, span], r.wd[:, span]))
            for cols in tiles:
                add(r.acc_x, cols, dot(r.xt[rs, span], r.vx[span, cols]))
        if "z" in what:
            for cols in part or tiles:
                add(r.acc_z, cols, dot(r.xt[rs, span], r.vz[span, cols]))

    def late_small(b):
        rs, span = rows_of(b), slice(cuts[2], cuts[3])
        x = r.xt.at[rs, span]
        r.mapped[rs, :] = silu(r.acc_m[rs, :] + dot(x[...], r.vb[span, :])).astype(BF16)
        v = r.acc_s[rs, :] + dot_nt(x[...], r.wd[:, span]) + r.bias[...]
        r.step[...] = jnp.maximum(v, 0.0) + jnp.log1p(jnp.exp(-jnp.abs(v)))

    def late_x(b, cols):
        rs, span = rows_of(b), slice(cuts[2], cuts[3])
        r.inner[rs, cols] = silu(r.acc_x[rs, cols] + dot(r.xt[rs, span], r.vx[span, cols])).astype(BF16)

    def late_z(b, part=None):
        rs, span = rows_of(b), slice(cuts[2], cuts[3])
        for cols in part or tiles:
            z = (r.acc_z[rs, cols] + dot(r.xt[rs, span], r.vz[span, cols])).astype(BF16).astype(F32)
            r.gate[rs, cols] = silu(z)

    def prepare(b):
        leaves, through = [], None
        for i in range(b * parts, (b + 1) * parts):
            rs = chunk_rows(i)
            stp = r.step[(i - b * parts) * CHUNK : (i - b * parts + 1) * CHUNK, :]
            decay = -stp * r.rate[...]
            high = decay.astype(BF16)
            rest = decay - high.astype(F32)
            middle = rest.astype(BF16)
            low = (rest - middle.astype(F32)).astype(BF16)
            cum = dot(r.tri[...], jnp.concatenate([high, middle, low], axis=0))
            last = cum[CHUNK - 1 :, :]
            before = r.before[i : i + 1, :]
            r.before[i + 1 : i + 2, :] = before + last
            r.cum[i] = cum
            r.cumt[i] = cum.T
            r.stept[i] = stp.T
            keep = r.same[rs, :] * jnp.exp2(last - cum) * stp
            r.keep[rs, :] = two_terms(keep)
            enter = r.alone[rs, :] * jnp.exp2(cum)
            outer = r.open[rs, :] * jnp.exp2(before + cum)
            r.enter[rs, :] = two_terms(enter)
            r.outer[rs, :] = two_terms(outer)
            passed = enter[CHUNK - 1 :, :]
            leaves = [value * passed for value in leaves] + [keep]
            through = passed if through is None else through * passed
            mapped_b, mapped_c = r.mapped[rs, :NSTATE], r.mapped[rs, NSTATE:]
            r.score[i] = r.mask[i] * dot_nt(mapped_c, mapped_b)
            turned = mapped_b.astype(F32).T.astype(BF16)
            r.turned[b, :, (i - b * parts) * CHUNK : (i - b * parts + 1) * CHUNK] = turned
        r.leave[...] = two_terms(jnp.concatenate(leaves, axis=0))
        slot = lax.broadcasted_iota(jnp.int32, (8, LANES), 0)
        ends = jnp.where(slot == 0, through, outer[CHUNK - 1 :, :])
        r.ends[...] = two_terms(ends)

    def down(c):
        return remote("seq", upper, r.leaving.at[c], r.arrived.at[c], r.c_send.at[0], r.c_recv.at[c])

    def widened(ref, rs, cols):
        return dot(ref[rs, :], r.widen[:, cols])

    def block_state(b, cols):
        rs = rows_of(b)
        scaled = (dot(r.leave[...], r.widen[:, cols]) * r.inner[rs, cols].astype(F32)).astype(BF16)
        new = dot(r.turned[b], scaled)
        if b:
            ends = dot(r.ends[...], r.widen[:, cols])
            r.through[:, cols] = ends
            new = new + ends[:1, :] * r.state[b - 1, :, cols]
        r.state[b, :, cols] = new

    def departures(cols):
        return range(cols.start // LANES, cols.stop // LANES)

    def leave_first(cols):
        for c in departures(cols):
            r.leaving[c] = r.state[blocks - 1, :, c * LANES : (c + 1) * LANES].astype(BF16)

        @pl.when((pos == 0) & (pos < chain - 1))
        def _():
            for c in departures(cols):
                down(c).start()

    def pass_on(c, cols):
        value = r.state[blocks - 1, :, cols] + r.through[1:2, cols] * r.arrived[c].astype(F32)
        r.leaving[c] = value.astype(BF16)
        down(c).start()

    def slot(at, picks):
        if picks and chain > at + 1:

            @pl.when(pos == at)
            def _():
                for c in picks:
                    down(c).wait_recv()
                    pass_on(c, slice(c * LANES, (c + 1) * LANES))

    def middle(i):
        b = i // parts
        rs = chunk_rows(i - 1)
        turned = r.turned[b, :, (i - 1 - b * parts) * CHUNK : (i - b * parts) * CHUNK]
        for cols in tiles:
            scaled = (widened(r.keep, rs, cols) * r.inner[rs, cols].astype(F32)).astype(BF16)
            new = dot(turned, scaled)
            if i > 1:
                passed = dot(r.enter[rs.stop - 16 : rs.stop, :], r.widen[:, cols])[15:, :]
                new = new + passed * (r.mid[...][:, cols] if (i - 1) % parts else r.state[b - 1, :, cols])
            r.mid[:, cols] = new

    def within(i):
        rs = chunk_rows(i)
        own_c = r.mapped[rs, NSTATE:]
        for cols in tiles:
            outer = dot(r.outer[rs, :], r.widen[:, cols])
            r.factor[rs, cols] = outer * r.gate[rs, cols]
            rest = r.skips[:1, cols] * r.inner[rs, cols].astype(F32)
            if i:
                start = r.mid[:, cols] if i % parts else r.state[i // parts - 1, :, cols]
                carried = dot(own_c, start.astype(BF16))
                rest = rest + dot(r.enter[rs, :], r.widen[:, cols]) * carried
            r.y[rs, cols] = rest
        for j in range(pairs):
            cols = slice(j * LANES, (j + 1) * LANES)
            x = r.inner[rs, cols]
            weights = []
            for h in range(per * j, per * (j + 1)):
                gap = r.cum[i, :, h : h + 1] - r.cumt[i, h : h + 1, :]
                weight = jnp.exp2(jnp.minimum(gap, 0.0)) * r.score[i] * r.stept[i, h : h + 1, :]
                weights.append(weight.astype(BF16))
            zero = jnp.zeros_like(x)
            split = jnp.concatenate([jnp.where(left, x, zero), jnp.where(left, zero, x)], axis=0)
            inside = dot(jnp.concatenate(weights, axis=1), split)
            r.y[rs, cols] = (r.y[rs, cols] + inside) * r.gate[rs, cols]

    r.before[...] = jnp.zeros_like(r.before)

    @pl.when(pos == 0)
    def _():
        r.arrived[...] = jnp.zeros_like(r.arrived)

    def relay(b):
        gathers[b][0].wait_recv()
        gathers[b][4].start()
        gathers[b][1].wait_recv()
        gathers[b][5].start()
        if b + 1 < blocks:
            for copy in gathers[b + 1][2:4]:
                copy.start()

    def pair_here(b, k):
        landing = r.xt.at[rows_of(b), place(k)]
        remote("head", across, landing, landing, r.g_send.at[0], r.g_recv.at[4 * b + k + 1]).wait_recv()

    def direct_here(b):
        pair_here(b, 1)

    def relayed_here(b):
        pair_here(b, 2)

    for copy in loads[0]:
        copy.wait()
    for copy in loads[3]:
        copy.start()
    projected(0, 0, "xz")
    if cores == 2:

        @pl.when(core == 1)
        def _():
            pl.semaphore_wait(r.go.at[0], 1)
            send_first()

    relay(0)
    for b in range(1, blocks):
        projected(b, 0, "xz")
    for k in (1, 2):
        for copy in loads[k]:
            copy.wait()
    for b in range(blocks):
        direct_here(b)
        projected(b, 1, "x")
        if b + 1 < blocks:
            relay(b + 1)
        if b == 0:
            projected(b, 1, "z")
            for copy in loads[3]:
                copy.wait()
            for copy in out_loads:
                copy.start()
        relayed_here(b)
        late_small(b)
        prepare(b)
        if b == 0 and cores == 2:

            @pl.when(core == 0)
            def _():
                pl.semaphore_signal(r.go.at[0], inc=1, device_id={"batch": other_core}, device_id_type=MESH)

        if b + 1 < blocks:
            for cols in tiles:
                late_x(b, cols)
            for cols in tiles:
                block_state(b, cols)
        else:
            late_x(b, tiles[0])
            for k, cols in enumerate(tiles):
                if k + 1 < len(tiles):
                    late_x(b, tiles[k + 1])
                block_state(b, cols)
                leave_first(cols)

    picks = [range(pairs * k // 10, pairs * (k + 1) // 10) for k in range(10)]

    def picked(low, high):
        return [c for k in range(low, high) for c in picks[k]]

    def both(one, two):
        slot(1, picked(*one))
        slot(2, picked(*two))

    late_z(0)
    both((0, 1), (0, 0))
    for b in range(1, blocks):
        projected(b, 1, "z", tiles[:some])
        both((1, 3), (0, 0))
        projected(b, 1, "z", tiles[some:])
    both((3, 5), (0, 0))
    for b in range(1, blocks):
        late_z(b, tiles[:some])
        both((5, 6), (0, 0))
        late_z(b, tiles[some:])
    both((6, 8), (0, 0))
    turns = {0: ((8, 10), (0, 1)), 1: ((0, 0), (1, 3)), 2: ((0, 0), (3, 5)), 3: ((0, 0), (5, 8)), 4: ((0, 0), (8, 10)), 5: ((0, 0), (0, 0))}
    turn = 0
    for i in range(chunks):
        if i % parts:
            middle(i)
            both(*turns[turn])
            turn += 1
        within(i)
        both(*turns[turn])
        turn += 1

    r.sums[...] = jnp.zeros_like(r.sums)

    def finish(cols):
        @pl.when((pos > 2) | ((pos > 0) & (pos == chain - 1)))
        def _():
            for c in departures(cols):
                down(c).wait_recv()

                @pl.when(pos < chain - 1)
                def _():
                    pass_on(c, slice(c * LANES, (c + 1) * LANES))

        arrived = jnp.concatenate([r.arrived[c] for c in departures(cols)], axis=1)
        carried = dot(r.mapped[:, NSTATE:], arrived)
        gated = r.y[:, cols] + r.factor[:, cols] * carried
        r.g[:, cols] = (gated * r.gain[:, cols]).astype(BF16)
        power = gated * gated
        total_power = r.sums[...]
        for k in range(0, cols.stop - cols.start, LANES):
            total_power = total_power + power[:, k : k + LANES]
        r.sums[...] = total_power

    for copy in out_loads:
        copy.wait()
    upper_half, lower_half = slice(0, rows // 2), slice(rows // 2, rows)
    ahead = tiles[-1].start
    for cols in tiles[:-1]:
        finish(cols)
    for k, rs in enumerate((upper_half, lower_half)):
        r.part[k] = dot(r.g[rs, :ahead], r.vw[0, :ahead, :])
    finish(tiles[-1])

    small = [
        remote("head", to, r.squares.at[k], r.others.at[k], r.q_send.at[0], r.q_recv.at[k])
        for k, to in enumerate((across, along))
    ]
    pieces = rows // 2 // half

    def place_of(p, k):
        return 2 * p + k if k < 2 else 2 * pieces if k < 4 else 2 * pieces + 1 + p

    scatters = [
        [
            remote("head", to, r.sent.at[pieces * k + p], r.back.at[pieces * k + p], r.o_send.at[0], r.o_recv.at[place_of(p, k)])
            for k, to in enumerate((across, along, across, along, along, across))
        ]
        for p in range(pieces)
    ]

    def put(p, k, value):
        r.sent[pieces * k + p] = value.astype(BF16)
        scatters[p][k].start()

    def piece(p):
        return slice(p * half, (p + 1) * half)

    def share(k, rs):
        return dot(r.g[rs, :], r.vw[k])

    def direct(k, source, rs):
        if source:
            value = share(source, rs)
        else:
            value = r.part[k] + dot(r.g[rs, ahead:], r.vw[0, ahead:, :])
        for p in range(pieces):
            put(p, k, value[piece(p), :])

    def joined(p):
        for k in (0, 1):
            scatters[p][k].wait_recv()
            put(p, 4 + k, r.part[k, piece(p), :] + r.back[pieces * k + p].astype(F32))

    direct(0, 0, upper_half)
    direct(1, 0, lower_half)
    spot = lax.broadcasted_iota(jnp.int32, (8, LANES), 0)
    squares = jnp.zeros((8, LANES), F32)
    for i in range(chunks):
        row = dot_nt(jnp.ones((8, LANES), F32), r.sums[chunk_rows(i), :], lax.Precision.HIGHEST)
        squares = jnp.where(spot == i, row, squares)
    r.squares[0] = squares
    small[0].start()
    direct(2, 1, upper_half)
    direct(3, 2, lower_half)
    r.part[0] = share(2, upper_half)
    r.part[1] = share(1, lower_half)
    for p in range(pieces):
        joined(p)
    small[0].wait_recv()
    r.squares[1] = r.squares[0] + r.others[0]
    small[1].start()
    own = r.y
    for rs in (upper_half, lower_half):
        own[rs, :depth] = share(3, rs)
    landing = r.back.at[2 * pieces : 4 * pieces]
    remote("head", across, landing, landing, r.o_send.at[0], r.o_recv.at[2 * pieces]).wait_recv()
    for k in (2, 3):
        base = (k - 2) * (rows // 2)
        for p in range(pieces):
            span = slice(base + p * half, base + (p + 1) * half)
            for i in range(depth // LANES):
                cols = slice(i * LANES, (i + 1) * LANES)
                own[span, cols] = own[span, cols] + r.back[pieces * k + p, :, cols].astype(F32)
    small[1].wait_recv()
    scale = lax.rsqrt((r.squares[1] + r.others[1]) / total + EPS)
    for i in range(chunks):
        r.sums[chunk_rows(i), :] = jnp.broadcast_to(scale[i : i + 1, :], (LANES, CHUNK)).T
    for p in range(pieces):
        landing = r.back.at[0:2]
        remote("head", across, landing, landing, r.o_send.at[0], r.o_recv.at[2 * pieces + 1 + p]).wait_recv()
        for k in (4, 5):
            base = (k - 4) * (rows // 2)
            span = slice(base + p * half, base + (p + 1) * half)
            for i in range(depth // LANES):
                cols = slice(i * LANES, (i + 1) * LANES)
                value = own[span, cols] + r.back[pieces * k + p, :, cols].astype(F32)
                out[span, cols] = (value * r.sums[span, :]).astype(BF16)

    for ref, send, recv in (
        (r.xt.at[:, : 3 * depth], r.g_send.at[0], r.g_recv.at[0]),
        (r.sent, r.o_send.at[0], r.o_recv.at[0]),
        (r.squares, r.q_send.at[0], r.q_recv.at[0]),
    ):
        remote("head", across, ref, ref, send, recv).wait_send()

    @pl.when(pos < chain - 1)
    def _():
        remote("seq", upper, r.leaving, r.leaving, r.c_send.at[0], r.c_recv.at[0]).wait_send()


def layer(chain, split, cores, tokens, resets, w_x, w_z, w_bc, w_dt, dt_bias, decay_rate, d_skip, norm_gain, w_out):
    rows, depth = tokens.shape
    width, heads, both = w_x.shape[1], w_dt.shape[1], w_bc.shape[1]
    blocks, pairs = rows // GROUP, width // LANES
    chunks = rows // CHUNK
    half = GROUP // 2
    vm, dma = pltpu.VMEM, pltpu.SemaphoreType.DMA
    scratch = dict(
        xt=vm((rows, 4 * depth), BF16),
        vx=vm((4 * depth, width), BF16),
        vz=vm((4 * depth, width), BF16),
        vb=vm((4 * depth, both), BF16),
        vw=vm((4, width, depth), BF16),
        wd=vm((LANES, 4 * depth), BF16),
        w_dt=vm((heads, 4 * depth), BF16),
        resets=vm((1, rows), jnp.int32),
        bias0=vm((1, heads), F32),
        rate0=vm((1, heads), F32),
        skip0=vm((1, heads), F32),
        bias=vm((1, LANES), F32),
        rate=vm((1, LANES), F32),
        skip=vm((1, LANES), F32),
        skips=vm((8, width), F32),
        gain0=vm((pairs, LANES), F32),
        gain=vm((1, width), F32),
        tri=vm((CHUNK, 3 * CHUNK), BF16),
        widen=vm((2 * LANES, width), BF16),
        mask=vm((chunks, CHUNK, CHUNK), F32),
        alone=vm((rows, LANES), F32),
        same=vm((rows, LANES), F32),
        open=vm((rows, LANES), F32),
        acc_x=vm((rows, width), F32),
        acc_z=vm((rows, width), F32),
        acc_m=vm((rows, both), F32),
        acc_s=vm((rows, LANES), F32),
        inner=vm((rows, width), BF16),
        gate=vm((rows, width), F32),
        mapped=vm((rows, both), BF16),
        turned=vm((blocks, NSTATE, GROUP), BF16),
        leave=vm((GROUP, 2 * LANES), BF16),
        ends=vm((8, 2 * LANES), BF16),
        through=vm((8, width), F32),
        mid=vm((NSTATE, width), F32),
        step=vm((GROUP, LANES), F32),
        before=vm((chunks + 1, LANES), F32),
        cum=vm((chunks, CHUNK, LANES), F32),
        cumt=vm((chunks, LANES, CHUNK), F32),
        stept=vm((chunks, LANES, CHUNK), F32),
        keep=vm((rows, 2 * LANES), BF16),
        enter=vm((rows, 2 * LANES), BF16),
        outer=vm((rows, 2 * LANES), BF16),
        score=vm((chunks, CHUNK, CHUNK), F32),
        state=vm((blocks, NSTATE, width), F32),
        arrived=vm((pairs, NSTATE, LANES), BF16),
        leaving=vm((pairs, NSTATE, LANES), BF16),
        y=vm((rows, width), F32),
        factor=vm((rows, width), F32),
        g=vm((rows, width), BF16),
        sums=vm((rows, LANES), F32),
        squares=vm((2, 8, LANES), F32),
        others=vm((2, 8, LANES), F32),
        part=vm((2, rows // 2, depth), F32),
        sent=vm((3 * rows // half, half, depth), BF16),
        back=vm((3 * rows // half, half, depth), BF16),
        small_load=dma((7,)),
        load=dma((9,)),
        g_send=dma((1,)),
        g_recv=dma((4 * blocks,)),
        c_send=dma((1,)),
        c_recv=dma((pairs,)),
        o_send=dma((1,)),
        o_recv=dma((3 * rows // 2 // half + 1,)),
        q_send=dma((1,)),
        q_recv=dma((2,)),
        go=pltpu.SemaphoreType.REGULAR((1,)),
    )
    return pl.pallas_call(
        functools.partial(kernel, chain, cores, float(width * split), tuple(scratch)),
        out_shape=pltpu.VMEM((rows, depth), BF16),
        in_specs=[ANY] * 11,
        out_specs=pl.BlockSpec(memory_space=pltpu.VMEM),
        scratch_shapes=list(scratch.values()),
        compiler_params=pltpu.CompilerParams(
            collective_id=0, has_side_effects=True, vmem_limit_bytes=60 * 1024 * 1024
        ),
    )(
        tokens, resets.reshape(1, rows), w_x, w_z, w_bc, w_dt.T, dt_bias.reshape(1, heads),
        decay_rate.reshape(1, heads), d_skip.reshape(1, heads), norm_gain.reshape(pairs, LANES), w_out,
    )


def solution(mesh):
    in_specs = (
        P(("batch", "seq"), "head"),
        P(("batch", "seq")),
        P(None, "head"),
        P(None, "head"),
        P(),
        P(None, "head"),
        P("head"),
        P("head"),
        P("head"),
        P("head"),
        P("head", None),
    )
    return jax.shard_map(
        functools.partial(layer, mesh.shape["seq"], mesh.shape["head"], mesh.shape["batch"]),
        mesh=mesh,
        in_specs=in_specs,
        out_specs=P(("batch", "seq"), "head"),
        check_vma=False,
    )
```

```python
import functools
import math

import jax
import jax.numpy as jnp
from jax import lax
from jax.experimental import pallas as pl
from jax.experimental.pallas import tpu as pltpu
from jax.sharding import PartitionSpec as P

HEADDIM = 64
NSTATE = 128
GROUP = 256
LANES = 128
CHUNK = 128
WIDE = 256
F32 = jnp.float32
BF16 = jnp.bfloat16
MESH = pl.DeviceIdType.MESH
ANY = pl.BlockSpec(memory_space=pl.ANY)
EPS = 1e-05
LOG2E = math.log2(math.e)


def peers():
    me = lax.axis_index("head")
    across = me + 1 - 2 * lax.rem(me, 2)
    along = lax.rem(me + 2, 4)
    corner = lax.rem(across + 2, 4)
    return me, across, along, corner


def remote(axis, to, src, dst, send, recv):
    return pltpu.make_async_remote_copy(
        src_ref=src, dst_ref=dst, send_sem=send, recv_sem=recv, device_id={axis: to}, device_id_type=MESH
    )


def silu(v):
    part = 0.5 * v
    return part + part * jnp.tanh(part)


class Scratch:
    def __init__(self, names, refs):
        for name, ref in zip(names, refs):
            setattr(self, name, ref)


def dot(a, b):
    return jnp.dot(a, b, preferred_element_type=F32)


def dot_nt(a, b, precision=None):
    return lax.dot_general(a, b, (((1,), (1,)), ((), ())), preferred_element_type=F32, precision=precision)


def two_terms(v):
    high = v.astype(BF16)
    return jnp.concatenate([high, (v - high.astype(F32)).astype(BF16)], axis=1)


def kernel(chain, cores, total, names, tok, resets, w_x, w_z, w_bc, w_dt, bias, rate, skip, gain, w_out, out, *refs):
    r = Scratch(names, refs)
    me, across, along, corner = peers()
    pos = lax.axis_index("seq")
    upper, lower = lax.rem(pos + 1, chain), lax.rem(pos + chain - 1, chain)
    rows, depth = tok.shape
    width = w_x.shape[1]
    heads = w_dt.shape[0]
    core, other_core = lax.axis_index("batch"), 1 - lax.axis_index("batch")
    leader = cores - 1
    blocks, pairs, per = rows // GROUP, width // LANES, LANES // HEADDIM
    half = GROUP // 2
    chunks, parts = rows // CHUNK, GROUP // CHUNK
    cuts = (0, depth // WIDE * WIDE, 3 * depth // WIDE * WIDE, 4 * depth)
    owners = (me, across, along, corner)
    tiles = [slice(i, min(i + WIDE, width)) for i in range(0, width, WIDE)]

    def span_of(owner):
        return pl.ds(pl.multiple_of(owner * depth, LANES), depth)

    def place(k):
        return slice(k * depth, (k + 1) * depth)

    def rows_of(b):
        return slice(b * GROUP, (b + 1) * GROUP)

    def chunk_rows(i):
        return slice(i * CHUNK, (i + 1) * CHUNK)

    own_tokens = pltpu.make_async_copy(tok, r.xt.at[:, place(0)], r.small_load.at[0])
    own_tokens.start()
    barrier = pltpu.get_barrier_semaphore()
    for other in (across, along):
        pl.semaphore_signal(barrier, inc=1, device_id={"head": other}, device_id_type=MESH)

    @pl.when(pos > 0)
    def _():
        pl.semaphore_signal(barrier, inc=1, device_id={"seq": lower}, device_id_type=MESH)

    if cores == 2:
        pl.semaphore_signal(barrier, inc=1, device_id={"batch": other_core}, device_id_type=MESH)
    smalls = [
        pltpu.make_async_copy(src, dst, r.small_load.at[1 + i])
        for i, (src, dst) in enumerate(
            (
                (resets, r.resets), (w_dt, r.w_dt), (bias, r.bias0), (rate, r.rate0), (skip, r.skip0), (gain, r.gain0),
            )
        )
    ]
    for copy in smalls:
        copy.start()
    loads = [
        (
            pltpu.make_async_copy(w_x.at[span_of(owner)], r.vx.at[place(k)], r.load.at[3 * (k % 3)]),
            pltpu.make_async_copy(w_z.at[span_of(owner)], r.vz.at[place(k)], r.load.at[3 * (k % 3) + 1]),
            pltpu.make_async_copy(w_bc.at[span_of(owner)], r.vb.at[place(k)], r.load.at[3 * (k % 3) + 2]),
        )
        for k, owner in enumerate(owners)
    ]
    order = (corner, across, along, me)
    out_loads = [
        pltpu.make_async_copy(w_out.at[:, span_of(owner)], r.vw.at[k], r.load.at[3 + k])
        for k, owner in enumerate(order)
    ]
    for group in loads[:3]:
        for copy in group:
            copy.start()

    gathers = []
    for b in range(blocks):
        lo = slice(b * GROUP, b * GROUP + half)
        hi = slice(b * GROUP + half, (b + 1) * GROUP)
        plan = (
            (across, r.xt.at[lo, place(0)], r.xt.at[lo, place(1)]),
            (along, r.xt.at[hi, place(0)], r.xt.at[hi, place(2)]),
            (across, r.xt.at[hi, place(0)], r.xt.at[hi, place(1)]),
            (along, r.xt.at[lo, place(0)], r.xt.at[lo, place(2)]),
            (along, r.xt.at[lo, place(1)], r.xt.at[lo, place(3)]),
            (across, r.xt.at[hi, place(2)], r.xt.at[hi, place(3)]),
        )
        gathers.append([
            remote("head", to, src, dst, r.g_send.at[0], r.g_recv.at[4 * b + min(i, 2) + i // 4])
            for i, (to, src, dst) in enumerate(plan)
        ])
    own_tokens.wait()

    @pl.when(pos < chain - 1)
    def _():
        pl.semaphore_wait(barrier, 3 + cores // 2)

    @pl.when(pos == chain - 1)
    def _():
        pl.semaphore_wait(barrier, 2 + cores // 2)


    def send_first():
        for copy in gathers[0][:4]:
            copy.start()
        for copies in gathers[1:]:
            for copy in copies[:2]:
                copy.start()

    @pl.when(core == leader)
    def _():
        send_first()

    ti = lax.broadcasted_iota(jnp.int32, (CHUNK, CHUNK), 0)
    si = lax.broadcasted_iota(jnp.int32, (CHUNK, CHUNK), 1)
    causal = ti >= si
    tri = jnp.where(causal, 1.0, 0.0).astype(F32)
    left = si < HEADDIM
    for k in range(3):
        r.tri[:, k * CHUNK : (k + 1) * CHUNK] = tri.astype(BF16)
    for cols in tiles:
        shape = (2 * LANES, cols.stop - cols.start)
        channel = lax.broadcasted_iota(jnp.int32, shape, 1) + cols.start
        source = lax.rem(lax.broadcasted_iota(jnp.int32, shape, 0), LANES)
        inside = (channel >= source * HEADDIM) & (channel < (source + 1) * HEADDIM)
        r.widen[:, cols] = jnp.where(inside, 1.0, 0.0).astype(BF16)
    for copy in smalls:
        copy.wait()
    r.rate[...] = jnp.zeros_like(r.rate)
    r.rate[:, :heads] = r.rate0[...] * LOG2E
    r.bias[...] = jnp.zeros_like(r.bias)
    r.bias[:, :heads] = r.bias0[...]
    r.skip[...] = jnp.zeros_like(r.skip)
    r.skip[:, :heads] = r.skip0[...]
    r.wd[...] = jnp.zeros_like(r.wd)
    for k, owner in enumerate(owners):
        r.wd[:heads, place(k)] = r.w_dt[:, span_of(owner)]
    for j in range(pairs):
        r.gain[:, j * LANES : (j + 1) * LANES] = r.gain0[j : j + 1, :]
    spare = jnp.broadcast_to(r.skip[...], (8, LANES))
    for cols in tiles:
        r.skips[:, cols] = dot(two_terms(spare), r.widen[:, cols])
    seen = jnp.zeros((1, LANES), F32)
    for i in range(chunks):
        rs = chunk_rows(i)
        starts = r.resets[:, rs].astype(F32)
        seg = jnp.broadcast_to(jnp.sum(tri * starts, axis=1, keepdims=True), (CHUNK, CHUNK))
        last = seg[CHUNK - 1 :, :]
        r.mask[i] = jnp.where(causal & (seg == seg.T), 1.0, 0.0)
        r.alone[rs, :] = jnp.where(seg == 0.0, 1.0, 0.0)
        r.same[rs, :] = jnp.where(seg == last, 1.0, 0.0)
        r.open[rs, :] = jnp.where(seg + seen == 0.0, 1.0, 0.0)
        seen = seen + last

    some = len(tiles) // 2

    def projected(b, k, what, part=None):
        rs, span = rows_of(b), slice(cuts[k], cuts[k + 1])

        def add(acc, cols, value):
            acc[rs, cols] = value if k == 0 else acc[rs, cols] + value

        if "x" in what:
            add(r.acc_m, slice(None), dot(r.xt[rs, span], r.vb[span, :]))
            add(r.acc_s, slice(None), dot_nt(r.xt[rs, span], r.wd[:, span]))
            for cols in tiles:
                add(r.acc_x, cols, dot(r.xt[rs, span], r.vx[span, cols]))
        if "z" in what:
            for cols in part or tiles:
                add(r.acc_z, cols, dot(r.xt[rs, span], r.vz[span, cols]))

    def late_small(b):
        rs, span = rows_of(b), slice(cuts[2], cuts[3])
        x = r.xt.at[rs, span]
        r.mapped[rs, :] = silu(r.acc_m[rs, :] + dot(x[...], r.vb[span, :])).astype(BF16)
        v = r.acc_s[rs, :] + dot_nt(x[...], r.wd[:, span]) + r.bias[...]
        r.step[...] = jnp.maximum(v, 0.0) + jnp.log1p(jnp.exp(-jnp.abs(v)))

    def late_x(b, cols):
        rs, span = rows_of(b), slice(cuts[2], cuts[3])
        r.inner[rs, cols] = silu(r.acc_x[rs, cols] + dot(r.xt[rs, span], r.vx[span, cols])).astype(BF16)

    def late_z(b, part=None):
        rs, span = rows_of(b), slice(cuts[2], cuts[3])
        for cols in part or tiles:
            z = (r.acc_z[rs, cols] + dot(r.xt[rs, span], r.vz[span, cols])).astype(BF16).astype(F32)
            r.gate[rs, cols] = silu(z)

    def prepare(b):
        leaves, through = [], None
        for i in range(b * parts, (b + 1) * parts):
            rs = chunk_rows(i)
            stp = r.step[(i - b * parts) * CHUNK : (i - b * parts + 1) * CHUNK, :]
            decay = -stp * r.rate[...]
            high = decay.astype(BF16)
            rest = decay - high.astype(F32)
            middle = rest.astype(BF16)
            low = (rest - middle.astype(F32)).astype(BF16)
            cum = dot(r.tri[...], jnp.concatenate([high, middle, low], axis=0))
            last = cum[CHUNK - 1 :, :]
            before = r.before[i : i + 1, :]
            r.before[i + 1 : i + 2, :] = before + last
            r.cum[i] = cum
            r.cumt[i] = cum.T
            r.stept[i] = stp.T
            keep = r.same[rs, :] * jnp.exp2(last - cum) * stp
            r.keep[rs, :] = two_terms(keep)
            enter = r.alone[rs, :] * jnp.exp2(cum)
            outer = r.open[rs, :] * jnp.exp2(before + cum)
            r.enter[rs, :] = two_terms(enter)
            r.outer[rs, :] = two_terms(outer)
            passed = enter[CHUNK - 1 :, :]
            leaves = [value * passed for value in leaves] + [keep]
            through = passed if through is None else through * passed
            mapped_b, mapped_c = r.mapped[rs, :NSTATE], r.mapped[rs, NSTATE:]
            r.score[i] = r.mask[i] * dot_nt(mapped_c, mapped_b)
            turned = mapped_b.astype(F32).T.astype(BF16)
            r.turned[b, :, (i - b * parts) * CHUNK : (i - b * parts + 1) * CHUNK] = turned
        r.leave[...] = two_terms(jnp.concatenate(leaves, axis=0))
        slot = lax.broadcasted_iota(jnp.int32, (8, LANES), 0)
        ends = jnp.where(slot == 0, through, outer[CHUNK - 1 :, :])
        r.ends[...] = two_terms(ends)

    def down(c):
        return remote("seq", upper, r.leaving.at[c], r.arrived.at[c], r.c_send.at[0], r.c_recv.at[c])

    def widened(ref, rs, cols):
        return dot(ref[rs, :], r.widen[:, cols])

    def block_state(b, cols):
        rs = rows_of(b)
        scaled = (dot(r.leave[...], r.widen[:, cols]) * r.inner[rs, cols].astype(F32)).astype(BF16)
        new = dot(r.turned[b], scaled)
        if b:
            ends = dot(r.ends[...], r.widen[:, cols])
            r.through[:, cols] = ends
            new = new + ends[:1, :] * r.state[b - 1, :, cols]
        r.state[b, :, cols] = new

    def departures(cols):
        return range(cols.start // LANES, cols.stop // LANES)

    def leave_first(cols):
        for c in departures(cols):
            r.leaving[c] = r.state[blocks - 1, :, c * LANES : (c + 1) * LANES].astype(BF16)

        @pl.when((pos == 0) & (pos < chain - 1))
        def _():
            for c in departures(cols):
                down(c).start()

    def pass_on(c, cols):
        value = r.state[blocks - 1, :, cols] + r.through[1:2, cols] * r.arrived[c].astype(F32)
        r.leaving[c] = value.astype(BF16)
        down(c).start()

    def slot(at, picks):
        if picks and chain > at + 1:

            @pl.when(pos == at)
            def _():
                for c in picks:
                    down(c).wait_recv()
                    pass_on(c, slice(c * LANES, (c + 1) * LANES))

    def middle(i):
        b = i // parts
        rs = chunk_rows(i - 1)
        turned = r.turned[b, :, (i - 1 - b * parts) * CHUNK : (i - b * parts) * CHUNK]
        for cols in tiles:
            scaled = (widened(r.keep, rs, cols) * r.inner[rs, cols].astype(F32)).astype(BF16)
            new = dot(turned, scaled)
            if i > 1:
                passed = dot(r.enter[rs.stop - 16 : rs.stop, :], r.widen[:, cols])[15:, :]
                new = new + passed * (r.mid[...][:, cols] if (i - 1) % parts else r.state[b - 1, :, cols])
            r.mid[:, cols] = new

    def within(i):
        rs = chunk_rows(i)
        own_c = r.mapped[rs, NSTATE:]
        for cols in tiles:
            outer = dot(r.outer[rs, :], r.widen[:, cols])
            r.factor[rs, cols] = outer * r.gate[rs, cols]
            rest = r.skips[:1, cols] * r.inner[rs, cols].astype(F32)
            if i:
                start = r.mid[:, cols] if i % parts else r.state[i // parts - 1, :, cols]
                carried = dot(own_c, start.astype(BF16))
                rest = rest + dot(r.enter[rs, :], r.widen[:, cols]) * carried
            r.y[rs, cols] = rest
        for j in range(pairs):
            cols = slice(j * LANES, (j + 1) * LANES)
            x = r.inner[rs, cols]
            weights = []
            for h in range(per * j, per * (j + 1)):
                gap = r.cum[i, :, h : h + 1] - r.cumt[i, h : h + 1, :]
                weight = jnp.exp2(jnp.minimum(gap, 0.0)) * r.score[i] * r.stept[i, h : h + 1, :]
                weights.append(weight.astype(BF16))
            zero = jnp.zeros_like(x)
            split = jnp.concatenate([jnp.where(left, x, zero), jnp.where(left, zero, x)], axis=0)
            inside = dot(jnp.concatenate(weights, axis=1), split)
            r.y[rs, cols] = (r.y[rs, cols] + inside) * r.gate[rs, cols]

    r.before[...] = jnp.zeros_like(r.before)

    @pl.when(pos == 0)
    def _():
        r.arrived[...] = jnp.zeros_like(r.arrived)

    def relay(b):
        gathers[b][0].wait_recv()
        gathers[b][4].start()
        gathers[b][1].wait_recv()
        gathers[b][5].start()
        if b + 1 < blocks:
            for copy in gathers[b + 1][2:4]:
                copy.start()

    def pair_here(b, k):
        landing = r.xt.at[rows_of(b), place(k)]
        remote("head", across, landing, landing, r.g_send.at[0], r.g_recv.at[4 * b + k + 1]).wait_recv()

    def direct_here(b):
        pair_here(b, 1)

    def relayed_here(b):
        pair_here(b, 2)

    for copy in loads[0]:
        copy.wait()
    for copy in loads[3]:
        copy.start()
    projected(0, 0, "xz")
    if cores == 2:

        @pl.when(core != leader)
        def _():
            pl.semaphore_wait(r.go.at[0], 1)
            send_first()

    relay(0)
    for b in range(1, blocks):
        projected(b, 0, "xz")
    for k in (1, 2):
        for copy in loads[k]:
            copy.wait()
    for b in range(blocks):
        direct_here(b)
        projected(b, 1, "x")
        if b + 1 < blocks:
            relay(b + 1)
        if b == 0:
            projected(b, 1, "z")
            for copy in loads[3]:
                copy.wait()
            for copy in out_loads:
                copy.start()
        relayed_here(b)
        late_small(b)
        prepare(b)
        if b == 0 and cores == 2:

            @pl.when(core == leader)
            def _():
                pl.semaphore_signal(r.go.at[0], inc=1, device_id={"batch": other_core}, device_id_type=MESH)

        if b + 1 < blocks:
            for cols in tiles:
                late_x(b, cols)
            for cols in tiles:
                block_state(b, cols)
        else:
            for low, high in ((0, 1), (1, 3), (3, len(tiles))):
                group = tiles[low:high]
                for cols in group:
                    late_x(b, cols)
                for cols in group:
                    block_state(b, cols)
                leave_first(slice(group[0].start, group[-1].stop))

    picks = [range(pairs * k // 10, pairs * (k + 1) // 10) for k in range(10)]

    def picked(low, high):
        return [c for k in range(low, high) for c in picks[k]]

    def both(one, two):
        slot(1, picked(*one))
        slot(2, picked(*two))

    late_z(0)
    both((0, 1), (0, 0))
    for b in range(1, blocks):
        projected(b, 1, "z", tiles[:some])
        both((1, 3), (0, 0))
        projected(b, 1, "z", tiles[some:])
    both((3, 5), (0, 0))
    for b in range(1, blocks):
        late_z(b, tiles[:some])
        both((5, 6), (0, 0))
        late_z(b, tiles[some:])
    both((6, 8), (0, 0))
    turns = {0: ((8, 10), (0, 1)), 1: ((0, 0), (1, 3)), 2: ((0, 0), (3, 5)), 3: ((0, 0), (5, 8)), 4: ((0, 0), (8, 10)), 5: ((0, 0), (0, 0))}
    turn = 0
    for i in range(chunks):
        if i % parts:
            middle(i)
            both(*turns[turn])
            turn += 1
        within(i)
        both(*turns[turn])
        turn += 1

    r.sums[...] = jnp.zeros_like(r.sums)

    def finish(cols):
        @pl.when((pos > 2) | ((pos > 0) & (pos == chain - 1)))
        def _():
            for c in departures(cols):
                down(c).wait_recv()

                @pl.when(pos < chain - 1)
                def _():
                    pass_on(c, slice(c * LANES, (c + 1) * LANES))

        arrived = jnp.concatenate([r.arrived[c] for c in departures(cols)], axis=1)
        carried = dot(r.mapped[:, NSTATE:], arrived)
        gated = r.y[:, cols] + r.factor[:, cols] * carried
        r.g[:, cols] = (gated * r.gain[:, cols]).astype(BF16)
        power = gated * gated
        total_power = r.sums[...]
        for k in range(0, cols.stop - cols.start, LANES):
            total_power = total_power + power[:, k : k + LANES]
        r.sums[...] = total_power

    for copy in out_loads:
        copy.wait()
    upper_half, lower_half = slice(0, rows // 2), slice(rows // 2, rows)
    ahead = tiles[-1].start
    for cols in tiles[:-1]:
        finish(cols)
    for k, rs in enumerate((upper_half, lower_half)):
        r.part[k] = dot(r.g[rs, :ahead], r.vw[0, :ahead, :])
    finish(tiles[-1])

    small = [
        remote("head", to, r.squares.at[k], r.others.at[k], r.q_send.at[0], r.q_recv.at[k])
        for k, to in enumerate((across, along))
    ]
    pieces = rows // 2 // half

    def place_of(p, k):
        return 2 * p + k if k < 2 else 2 * pieces if k < 4 else 2 * pieces + 1 + p

    scatters = [
        [
            remote("head", to, r.sent.at[pieces * k + p], r.back.at[pieces * k + p], r.o_send.at[0], r.o_recv.at[place_of(p, k)])
            for k, to in enumerate((across, along, across, along, along, across))
        ]
        for p in range(pieces)
    ]

    def put(p, k, value):
        r.sent[pieces * k + p] = value.astype(BF16)
        scatters[p][k].start()

    def piece(p):
        return slice(p * half, (p + 1) * half)

    def share(k, rs):
        return dot(r.g[rs, :], r.vw[k])

    def direct(k, source, rs):
        if source:
            value = share(source, rs)
        else:
            value = r.part[k] + dot(r.g[rs, ahead:], r.vw[0, ahead:, :])
        for p in range(pieces):
            put(p, k, value[piece(p), :])

    def joined(p):
        for k in (0, 1):
            scatters[p][k].wait_recv()
            put(p, 4 + k, r.part[k, piece(p), :] + r.back[pieces * k + p].astype(F32))

    direct(0, 0, upper_half)
    direct(1, 0, lower_half)
    spot = lax.broadcasted_iota(jnp.int32, (8, LANES), 0)
    squares = jnp.zeros((8, LANES), F32)
    for i in range(chunks):
        row = dot_nt(jnp.ones((8, LANES), F32), r.sums[chunk_rows(i), :], lax.Precision.HIGHEST)
        squares = jnp.where(spot == i, row, squares)
    r.squares[0] = squares
    small[0].start()
    direct(2, 1, upper_half)
    direct(3, 2, lower_half)
    r.part[0] = share(2, upper_half)
    r.part[1] = share(1, lower_half)
    for p in range(pieces):
        joined(p)
    small[0].wait_recv()
    r.squares[1] = r.squares[0] + r.others[0]
    small[1].start()
    own = r.y
    for rs in (upper_half, lower_half):
        own[rs, :depth] = share(3, rs)
    landing = r.back.at[2 * pieces : 4 * pieces]
    remote("head", across, landing, landing, r.o_send.at[0], r.o_recv.at[2 * pieces]).wait_recv()
    for k in (2, 3):
        base = (k - 2) * (rows // 2)
        for p in range(pieces):
            span = slice(base + p * half, base + (p + 1) * half)
            for i in range(depth // LANES):
                cols = slice(i * LANES, (i + 1) * LANES)
                own[span, cols] = own[span, cols] + r.back[pieces * k + p, :, cols].astype(F32)
    small[1].wait_recv()
    scale = lax.rsqrt((r.squares[1] + r.others[1]) / total + EPS)
    for i in range(chunks):
        r.sums[chunk_rows(i), :] = jnp.broadcast_to(scale[i : i + 1, :], (LANES, CHUNK)).T
    for p in range(pieces):
        landing = r.back.at[0:2]
        remote("head", across, landing, landing, r.o_send.at[0], r.o_recv.at[2 * pieces + 1 + p]).wait_recv()
        for k in (4, 5):
            base = (k - 4) * (rows // 2)
            span = slice(base + p * half, base + (p + 1) * half)
            for i in range(depth // LANES):
                cols = slice(i * LANES, (i + 1) * LANES)
                value = own[span, cols] + r.back[pieces * k + p, :, cols].astype(F32)
                out[span, cols] = (value * r.sums[span, :]).astype(BF16)

    for ref, send, recv in (
        (r.xt.at[:, : 3 * depth], r.g_send.at[0], r.g_recv.at[0]),
        (r.sent, r.o_send.at[0], r.o_recv.at[0]),
        (r.squares, r.q_send.at[0], r.q_recv.at[0]),
    ):
        remote("head", across, ref, ref, send, recv).wait_send()

    @pl.when(pos < chain - 1)
    def _():
        remote("seq", upper, r.leaving, r.leaving, r.c_send.at[0], r.c_recv.at[0]).wait_send()


def layer(chain, split, cores, tokens, resets, w_x, w_z, w_bc, w_dt, dt_bias, decay_rate, d_skip, norm_gain, w_out):
    rows, depth = tokens.shape
    width, heads, both = w_x.shape[1], w_dt.shape[1], w_bc.shape[1]
    blocks, pairs = rows // GROUP, width // LANES
    chunks = rows // CHUNK
    half = GROUP // 2
    vm, dma = pltpu.VMEM, pltpu.SemaphoreType.DMA
    scratch = dict(
        xt=vm((rows, 4 * depth), BF16),
        vx=vm((4 * depth, width), BF16),
        vz=vm((4 * depth, width), BF16),
        vb=vm((4 * depth, both), BF16),
        vw=vm((4, width, depth), BF16),
        wd=vm((LANES, 4 * depth), BF16),
        w_dt=vm((heads, 4 * depth), BF16),
        resets=vm((1, rows), jnp.int32),
        bias0=vm((1, heads), F32),
        rate0=vm((1, heads), F32),
        skip0=vm((1, heads), F32),
        bias=vm((1, LANES), F32),
        rate=vm((1, LANES), F32),
        skip=vm((1, LANES), F32),
        skips=vm((8, width), F32),
        gain0=vm((pairs, LANES), F32),
        gain=vm((1, width), F32),
        tri=vm((CHUNK, 3 * CHUNK), BF16),
        widen=vm((2 * LANES, width), BF16),
        mask=vm((chunks, CHUNK, CHUNK), F32),
        alone=vm((rows, LANES), F32),
        same=vm((rows, LANES), F32),
        open=vm((rows, LANES), F32),
        acc_x=vm((rows, width), F32),
        acc_z=vm((rows, width), F32),
        acc_m=vm((rows, both), F32),
        acc_s=vm((rows, LANES), F32),
        inner=vm((rows, width), BF16),
        gate=vm((rows, width), F32),
        mapped=vm((rows, both), BF16),
        turned=vm((blocks, NSTATE, GROUP), BF16),
        leave=vm((GROUP, 2 * LANES), BF16),
        ends=vm((8, 2 * LANES), BF16),
        through=vm((8, width), F32),
        mid=vm((NSTATE, width), F32),
        step=vm((GROUP, LANES), F32),
        before=vm((chunks + 1, LANES), F32),
        cum=vm((chunks, CHUNK, LANES), F32),
        cumt=vm((chunks, LANES, CHUNK), F32),
        stept=vm((chunks, LANES, CHUNK), F32),
        keep=vm((rows, 2 * LANES), BF16),
        enter=vm((rows, 2 * LANES), BF16),
        outer=vm((rows, 2 * LANES), BF16),
        score=vm((chunks, CHUNK, CHUNK), F32),
        state=vm((blocks, NSTATE, width), F32),
        arrived=vm((pairs, NSTATE, LANES), BF16),
        leaving=vm((pairs, NSTATE, LANES), BF16),
        y=vm((rows, width), F32),
        factor=vm((rows, width), F32),
        g=vm((rows, width), BF16),
        sums=vm((rows, LANES), F32),
        squares=vm((2, 8, LANES), F32),
        others=vm((2, 8, LANES), F32),
        part=vm((2, rows // 2, depth), F32),
        sent=vm((3 * rows // half, half, depth), BF16),
        back=vm((3 * rows // half, half, depth), BF16),
        small_load=dma((7,)),
        load=dma((9,)),
        g_send=dma((1,)),
        g_recv=dma((4 * blocks,)),
        c_send=dma((1,)),
        c_recv=dma((pairs,)),
        o_send=dma((1,)),
        o_recv=dma((3 * rows // 2 // half + 1,)),
        q_send=dma((1,)),
        q_recv=dma((2,)),
        go=pltpu.SemaphoreType.REGULAR((1,)),
    )
    return pl.pallas_call(
        functools.partial(kernel, chain, cores, float(width * split), tuple(scratch)),
        out_shape=pltpu.VMEM((rows, depth), BF16),
        in_specs=[ANY] * 11,
        out_specs=pl.BlockSpec(memory_space=pltpu.VMEM),
        scratch_shapes=list(scratch.values()),
        compiler_params=pltpu.CompilerParams(
            collective_id=0, has_side_effects=True, vmem_limit_bytes=60 * 1024 * 1024
        ),
    )(
        tokens, resets.reshape(1, rows), w_x, w_z, w_bc, w_dt.T, dt_bias.reshape(1, heads),
        decay_rate.reshape(1, heads), d_skip.reshape(1, heads), norm_gain.reshape(pairs, LANES), w_out,
    )


def solution(mesh):
    in_specs = (
        P(("batch", "seq"), "head"),
        P(("batch", "seq")),
        P(None, "head"),
        P(None, "head"),
        P(),
        P(None, "head"),
        P("head"),
        P("head"),
        P("head"),
        P("head"),
        P("head", None),
    )
    return jax.shard_map(
        functools.partial(layer, mesh.shape["seq"], mesh.shape["head"], mesh.shape["batch"]),
        mesh=mesh,
        in_specs=in_specs,
        out_specs=P(("batch", "seq"), "head"),
        check_vma=False,
    )
```

```python
import functools
import math

import jax
import jax.numpy as jnp
from jax import lax
from jax.experimental import pallas as pl
from jax.experimental.pallas import tpu as pltpu
from jax.sharding import PartitionSpec as P

HEADDIM = 64
NSTATE = 128
GROUP = 256
LANES = 128
CHUNK = 128
WIDE = 256
F32 = jnp.float32
BF16 = jnp.bfloat16
MESH = pl.DeviceIdType.MESH
ANY = pl.BlockSpec(memory_space=pl.ANY)
EPS = 1e-05
LOG2E = math.log2(math.e)


def peers():
    me = lax.axis_index("head")
    across = me + 1 - 2 * lax.rem(me, 2)
    along = lax.rem(me + 2, 4)
    corner = lax.rem(across + 2, 4)
    return me, across, along, corner


def remote(axis, to, src, dst, send, recv):
    return pltpu.make_async_remote_copy(
        src_ref=src, dst_ref=dst, send_sem=send, recv_sem=recv, device_id={axis: to}, device_id_type=MESH
    )


def silu(v):
    part = 0.5 * v
    return part + part * jnp.tanh(part)


class Scratch:
    def __init__(self, names, refs):
        for name, ref in zip(names, refs):
            setattr(self, name, ref)


def dot(a, b):
    return jnp.dot(a, b, preferred_element_type=F32)


def dot_nt(a, b, precision=None):
    return lax.dot_general(a, b, (((1,), (1,)), ((), ())), preferred_element_type=F32, precision=precision)


def two_terms(v):
    high = v.astype(BF16)
    return jnp.concatenate([high, (v - high.astype(F32)).astype(BF16)], axis=1)


def kernel(chain, cores, total, names, tok, resets, w_x, w_z, w_bc, w_dt, bias, rate, skip, gain, w_out, out, *refs):
    r = Scratch(names, refs)
    me, across, along, corner = peers()
    pos = lax.axis_index("seq")
    upper, lower = lax.rem(pos + 1, chain), lax.rem(pos + chain - 1, chain)
    rows, depth = tok.shape
    width = w_x.shape[1]
    heads = w_dt.shape[0]
    core, other_core = lax.axis_index("batch"), 1 - lax.axis_index("batch")
    leader = cores - 1
    blocks, pairs, per = rows // GROUP, width // LANES, LANES // HEADDIM
    half = GROUP // 2
    chunks, parts = rows // CHUNK, GROUP // CHUNK
    cuts = (0, depth // WIDE * WIDE, 3 * depth // WIDE * WIDE, 4 * depth)
    owners = (me, across, along, corner)
    tiles = [slice(i, min(i + WIDE, width)) for i in range(0, width, WIDE)]

    def span_of(owner):
        return pl.ds(pl.multiple_of(owner * depth, LANES), depth)

    def place(k):
        return slice(k * depth, (k + 1) * depth)

    def rows_of(b):
        return slice(b * GROUP, (b + 1) * GROUP)

    def chunk_rows(i):
        return slice(i * CHUNK, (i + 1) * CHUNK)

    own_tokens = pltpu.make_async_copy(tok, r.xt.at[:, place(0)], r.small_load.at[0])
    own_tokens.start()
    barrier = pltpu.get_barrier_semaphore()
    for other in (across, along):
        pl.semaphore_signal(barrier, inc=1, device_id={"head": other}, device_id_type=MESH)

    @pl.when(pos > 0)
    def _():
        pl.semaphore_signal(barrier, inc=1, device_id={"seq": lower}, device_id_type=MESH)

    if cores == 2:
        pl.semaphore_signal(barrier, inc=1, device_id={"batch": other_core}, device_id_type=MESH)
    smalls = [
        pltpu.make_async_copy(src, dst, r.small_load.at[1 + i])
        for i, (src, dst) in enumerate(
            (
                (resets, r.resets), (w_dt, r.w_dt), (bias, r.bias0), (rate, r.rate0), (skip, r.skip0), (gain, r.gain0),
            )
        )
    ]
    for copy in smalls:
        copy.start()
    loads = [
        (
            pltpu.make_async_copy(w_x.at[span_of(owner)], r.vx.at[place(k)], r.load.at[3 * (k % 3)]),
            pltpu.make_async_copy(w_z.at[span_of(owner)], r.vz.at[place(k)], r.load.at[3 * (k % 3) + 1]),
            pltpu.make_async_copy(w_bc.at[span_of(owner)], r.vb.at[place(k)], r.load.at[3 * (k % 3) + 2]),
        )
        for k, owner in enumerate(owners)
    ]
    order = (corner, across, along, me)
    out_loads = [
        pltpu.make_async_copy(w_out.at[:, span_of(owner)], r.vw.at[k], r.load.at[3 + k])
        for k, owner in enumerate(order)
    ]
    for group in loads[:3]:
        for copy in group:
            copy.start()

    gathers = []
    for b in range(blocks):
        lo = slice(b * GROUP, b * GROUP + half)
        hi = slice(b * GROUP + half, (b + 1) * GROUP)
        plan = (
            (across, r.xt.at[lo, place(0)], r.xt.at[lo, place(1)]),
            (along, r.xt.at[hi, place(0)], r.xt.at[hi, place(2)]),
            (across, r.xt.at[hi, place(0)], r.xt.at[hi, place(1)]),
            (along, r.xt.at[lo, place(0)], r.xt.at[lo, place(2)]),
            (along, r.xt.at[lo, place(1)], r.xt.at[lo, place(3)]),
            (across, r.xt.at[hi, place(2)], r.xt.at[hi, place(3)]),
        )
        gathers.append([
            remote("head", to, src, dst, r.g_send.at[0], r.g_recv.at[4 * b + min(i, 2) + i // 4])
            for i, (to, src, dst) in enumerate(plan)
        ])
    own_tokens.wait()

    @pl.when(pos < chain - 1)
    def _():
        pl.semaphore_wait(barrier, 3 + cores // 2)

    @pl.when(pos == chain - 1)
    def _():
        pl.semaphore_wait(barrier, 2 + cores // 2)


    def send_first():
        for copy in gathers[0][:4]:
            copy.start()
        for copies in gathers[1:]:
            for copy in copies[:2]:
                copy.start()

    @pl.when(core == leader)
    def _():
        send_first()

    ti = lax.broadcasted_iota(jnp.int32, (CHUNK, CHUNK), 0)
    si = lax.broadcasted_iota(jnp.int32, (CHUNK, CHUNK), 1)
    causal = ti >= si
    tri = jnp.where(causal, 1.0, 0.0).astype(F32)
    left = si < HEADDIM
    for k in range(3):
        r.tri[:, k * CHUNK : (k + 1) * CHUNK] = tri.astype(BF16)
    for cols in tiles:
        shape = (2 * LANES, cols.stop - cols.start)
        channel = lax.broadcasted_iota(jnp.int32, shape, 1) + cols.start
        source = lax.rem(lax.broadcasted_iota(jnp.int32, shape, 0), LANES)
        inside = (channel >= source * HEADDIM) & (channel < (source + 1) * HEADDIM)
        r.widen[:, cols] = jnp.where(inside, 1.0, 0.0).astype(BF16)
    for copy in smalls:
        copy.wait()
    r.rate[...] = jnp.zeros_like(r.rate)
    r.rate[:, :heads] = r.rate0[...] * LOG2E
    r.bias[...] = jnp.zeros_like(r.bias)
    r.bias[:, :heads] = r.bias0[...]
    r.skip[...] = jnp.zeros_like(r.skip)
    r.skip[:, :heads] = r.skip0[...]
    r.wd[...] = jnp.zeros_like(r.wd)
    for k, owner in enumerate(owners):
        r.wd[:heads, place(k)] = r.w_dt[:, span_of(owner)]
    for j in range(pairs):
        r.gain[:, j * LANES : (j + 1) * LANES] = r.gain0[j : j + 1, :]
    spare = jnp.broadcast_to(r.skip[...], (8, LANES))
    for cols in tiles:
        r.skips[:, cols] = dot(two_terms(spare), r.widen[:, cols])
    seen = jnp.zeros((1, LANES), F32)
    for i in range(chunks):
        rs = chunk_rows(i)
        starts = r.resets[:, rs].astype(F32)
        seg = jnp.broadcast_to(jnp.sum(tri * starts, axis=1, keepdims=True), (CHUNK, CHUNK))
        last = seg[CHUNK - 1 :, :]
        r.mask[i] = jnp.where(causal & (seg == seg.T), 1.0, 0.0)
        r.alone[rs, :] = jnp.where(seg == 0.0, 1.0, 0.0)
        r.same[rs, :] = jnp.where(seg == last, 1.0, 0.0)
        r.open[rs, :] = jnp.where(seg + seen == 0.0, 1.0, 0.0)
        seen = seen + last

    some = len(tiles) // 2

    def projected(b, k, what, part=None):
        rs, span = rows_of(b), slice(cuts[k], cuts[k + 1])

        def add(acc, cols, value):
            acc[rs, cols] = value if k == 0 else acc[rs, cols] + value

        if "x" in what:
            add(r.acc_m, slice(None), dot(r.xt[rs, span], r.vb[span, :]))
            add(r.acc_s, slice(None), dot_nt(r.xt[rs, span], r.wd[:, span]))
            for cols in tiles:
                add(r.acc_x, cols, dot(r.xt[rs, span], r.vx[span, cols]))
        if "z" in what:
            for cols in part or tiles:
                add(r.acc_z, cols, dot(r.xt[rs, span], r.vz[span, cols]))

    def late_small(b):
        rs, span = rows_of(b), slice(cuts[2], cuts[3])
        x = r.xt.at[rs, span]
        r.mapped[rs, :] = silu(r.acc_m[rs, :] + dot(x[...], r.vb[span, :])).astype(BF16)
        v = r.acc_s[rs, :] + dot_nt(x[...], r.wd[:, span]) + r.bias[...]
        r.step[...] = jnp.maximum(v, 0.0) + jnp.log1p(jnp.exp(-jnp.abs(v)))

    def late_x(b, cols):
        rs, span = rows_of(b), slice(cuts[2], cuts[3])
        r.inner[rs, cols] = silu(r.acc_x[rs, cols] + dot(r.xt[rs, span], r.vx[span, cols])).astype(BF16)

    def late_z(b, part=None):
        rs, span = rows_of(b), slice(cuts[2], cuts[3])
        for cols in part or tiles:
            z = (r.acc_z[rs, cols] + dot(r.xt[rs, span], r.vz[span, cols])).astype(BF16).astype(F32)
            r.gate[rs, cols] = silu(z)

    def prepare(b):
        leaves, through = [], None
        for i in range(b * parts, (b + 1) * parts):
            rs = chunk_rows(i)
            stp = r.step[(i - b * parts) * CHUNK : (i - b * parts + 1) * CHUNK, :]
            decay = -stp * r.rate[...]
            high = decay.astype(BF16)
            rest = decay - high.astype(F32)
            middle = rest.astype(BF16)
            low = (rest - middle.astype(F32)).astype(BF16)
            cum = dot(r.tri[...], jnp.concatenate([high, middle, low], axis=0))
            last = cum[CHUNK - 1 :, :]
            before = r.before[i : i + 1, :]
            r.before[i + 1 : i + 2, :] = before + last
            r.cum[i] = cum
            r.cumt[i] = cum.T
            r.stept[i] = stp.T
            keep = r.same[rs, :] * jnp.exp2(last - cum) * stp
            r.keep[rs, :] = two_terms(keep)
            enter = r.alone[rs, :] * jnp.exp2(cum)
            outer = r.open[rs, :] * jnp.exp2(before + cum)
            r.enter[rs, :] = two_terms(enter)
            r.outer[rs, :] = two_terms(outer)
            passed = enter[CHUNK - 1 :, :]
            leaves = [value * passed for value in leaves] + [keep]
            through = passed if through is None else through * passed
            mapped_b, mapped_c = r.mapped[rs, :NSTATE], r.mapped[rs, NSTATE:]
            r.score[i] = r.mask[i] * dot_nt(mapped_c, mapped_b)
            turned = mapped_b.astype(F32).T.astype(BF16)
            r.turned[b, :, (i - b * parts) * CHUNK : (i - b * parts + 1) * CHUNK] = turned
        r.leave[...] = two_terms(jnp.concatenate(leaves, axis=0))
        slot = lax.broadcasted_iota(jnp.int32, (8, LANES), 0)
        ends = jnp.where(slot == 0, through, outer[CHUNK - 1 :, :])
        r.ends[...] = two_terms(ends)

    def down(c):
        return remote("seq", upper, r.leaving.at[c], r.arrived.at[c], r.c_send.at[0], r.c_recv.at[c])

    def widened(ref, rs, cols):
        return dot(ref[rs, :], r.widen[:, cols])

    def block_state(b, cols):
        rs = rows_of(b)
        scaled = (dot(r.leave[...], r.widen[:, cols]) * r.inner[rs, cols].astype(F32)).astype(BF16)
        new = dot(r.turned[b], scaled)
        if b:
            ends = dot(r.ends[...], r.widen[:, cols])
            r.through[:, cols] = ends
            new = new + ends[:1, :] * r.state[b - 1, :, cols]
        r.state[b, :, cols] = new

    def departures(cols):
        return range(cols.start // LANES, cols.stop // LANES)

    def leave_first(cols):
        for c in departures(cols):
            r.leaving[c] = r.state[blocks - 1, :, c * LANES : (c + 1) * LANES].astype(BF16)

        @pl.when((pos == 0) & (pos < chain - 1))
        def _():
            for c in departures(cols):
                down(c).start()

    def pass_on(c, cols):
        value = r.state[blocks - 1, :, cols] + r.through[1:2, cols] * r.arrived[c].astype(F32)
        r.leaving[c] = value.astype(BF16)
        down(c).start()

    def slot(at, picks):
        if picks and chain > at + 1:

            @pl.when(pos == at)
            def _():
                for c in picks:
                    down(c).wait_recv()
                    pass_on(c, slice(c * LANES, (c + 1) * LANES))

    def middle(i):
        b = i // parts
        rs = chunk_rows(i - 1)
        turned = r.turned[b, :, (i - 1 - b * parts) * CHUNK : (i - b * parts) * CHUNK]
        for cols in tiles:
            scaled = (widened(r.keep, rs, cols) * r.inner[rs, cols].astype(F32)).astype(BF16)
            new = dot(turned, scaled)
            if i > 1:
                passed = dot(r.enter[rs.stop - 16 : rs.stop, :], r.widen[:, cols])[15:, :]
                new = new + passed * (r.mid[...][:, cols] if (i - 1) % parts else r.state[b - 1, :, cols])
            r.mid[:, cols] = new

    def within(i):
        rs = chunk_rows(i)
        own_c = r.mapped[rs, NSTATE:]
        for cols in tiles:
            outer = dot(r.outer[rs, :], r.widen[:, cols])
            r.factor[rs, cols] = outer * r.gate[rs, cols]
            rest = r.skips[:1, cols] * r.inner[rs, cols].astype(F32)
            if i:
                start = r.mid[:, cols] if i % parts else r.state[i // parts - 1, :, cols]
                carried = dot(own_c, start.astype(BF16))
                rest = rest + dot(r.enter[rs, :], r.widen[:, cols]) * carried
            r.y[rs, cols] = rest
        for j in range(pairs):
            cols = slice(j * LANES, (j + 1) * LANES)
            x = r.inner[rs, cols]
            weights = []
            for h in range(per * j, per * (j + 1)):
                gap = r.cum[i, :, h : h + 1] - r.cumt[i, h : h + 1, :]
                weight = jnp.exp2(jnp.minimum(gap, 0.0)) * r.score[i] * r.stept[i, h : h + 1, :]
                weights.append(weight.astype(BF16))
            zero = jnp.zeros_like(x)
            split = jnp.concatenate([jnp.where(left, x, zero), jnp.where(left, zero, x)], axis=0)
            inside = dot(jnp.concatenate(weights, axis=1), split)
            r.y[rs, cols] = (r.y[rs, cols] + inside) * r.gate[rs, cols]

    r.before[...] = jnp.zeros_like(r.before)

    @pl.when(pos == 0)
    def _():
        r.arrived[...] = jnp.zeros_like(r.arrived)

    def relay(b):
        gathers[b][0].wait_recv()
        gathers[b][4].start()
        gathers[b][1].wait_recv()
        gathers[b][5].start()
        if b + 1 < blocks:
            for copy in gathers[b + 1][2:4]:
                copy.start()

    def pair_here(b, k):
        landing = r.xt.at[rows_of(b), place(k)]
        remote("head", across, landing, landing, r.g_send.at[0], r.g_recv.at[4 * b + k + 1]).wait_recv()

    def direct_here(b):
        pair_here(b, 1)

    def relayed_here(b):
        pair_here(b, 2)

    for copy in loads[0]:
        copy.wait()
    for copy in loads[3]:
        copy.start()
    projected(0, 0, "xz")
    if cores == 2:

        @pl.when(core != leader)
        def _():
            pl.semaphore_wait(r.go.at[0], 1)
            send_first()

    relay(0)
    for b in range(1, blocks):
        projected(b, 0, "xz")
    for k in (1, 2):
        for copy in loads[k]:
            copy.wait()
    for b in range(blocks):
        direct_here(b)
        projected(b, 1, "x")
        if b + 1 < blocks:
            relay(b + 1)
        if b == 0:
            projected(b, 1, "z")
            for copy in loads[3]:
                copy.wait()
            for copy in out_loads:
                copy.start()
        relayed_here(b)
        if b == 0 and cores == 2:

            @pl.when(core == leader)
            def _():
                pl.semaphore_signal(r.go.at[0], inc=1, device_id={"batch": other_core}, device_id_type=MESH)

        late_small(b)
        prepare(b)
        if b + 1 < blocks:
            for cols in tiles:
                late_x(b, cols)
            for cols in tiles:
                block_state(b, cols)
        else:
            for low, high in ((0, 1), (1, 3), (3, len(tiles))):
                group = tiles[low:high]
                for cols in group:
                    late_x(b, cols)
                for cols in group:
                    block_state(b, cols)
                leave_first(slice(group[0].start, group[-1].stop))

    picks = [range(pairs * k // 10, pairs * (k + 1) // 10) for k in range(10)]

    def picked(low, high):
        return [c for k in range(low, high) for c in picks[k]]

    def both(one, two):
        slot(1, picked(*one))
        slot(2, picked(*two))

    late_z(0)
    both((0, 1), (0, 0))
    for b in range(1, blocks):
        projected(b, 1, "z", tiles[:some])
        both((1, 3), (0, 0))
        projected(b, 1, "z", tiles[some:])
    both((3, 5), (0, 0))
    for b in range(1, blocks):
        late_z(b, tiles[:some])
        both((5, 6), (0, 0))
        late_z(b, tiles[some:])
    both((6, 8), (0, 0))
    turns = {0: ((8, 10), (0, 1)), 1: ((0, 0), (1, 3)), 2: ((0, 0), (3, 5)), 3: ((0, 0), (5, 8)), 4: ((0, 0), (8, 10)), 5: ((0, 0), (0, 0))}
    turn = 0
    for i in range(chunks):
        if i % parts:
            middle(i)
            both(*turns[turn])
            turn += 1
        within(i)
        both(*turns[turn])
        turn += 1

    r.sums[...] = jnp.zeros_like(r.sums)

    def finish(cols):
        @pl.when((pos > 2) | ((pos > 0) & (pos == chain - 1)))
        def _():
            for c in departures(cols):
                down(c).wait_recv()

                @pl.when(pos < chain - 1)
                def _():
                    pass_on(c, slice(c * LANES, (c + 1) * LANES))

        arrived = jnp.concatenate([r.arrived[c] for c in departures(cols)], axis=1)
        carried = dot(r.mapped[:, NSTATE:], arrived)
        gated = r.y[:, cols] + r.factor[:, cols] * carried
        r.g[:, cols] = (gated * r.gain[:, cols]).astype(BF16)
        power = gated * gated
        total_power = r.sums[...]
        for k in range(0, cols.stop - cols.start, LANES):
            total_power = total_power + power[:, k : k + LANES]
        r.sums[...] = total_power

    for copy in out_loads:
        copy.wait()
    upper_half, lower_half = slice(0, rows // 2), slice(rows // 2, rows)
    ahead = tiles[-1].start
    for cols in tiles[:-1]:
        finish(cols)
    for k, rs in enumerate((upper_half, lower_half)):
        r.part[k] = dot(r.g[rs, :ahead], r.vw[0, :ahead, :])
    finish(tiles[-1])

    small = [
        remote("head", to, r.squares.at[k], r.others.at[k], r.q_send.at[0], r.q_recv.at[k])
        for k, to in enumerate((across, along))
    ]
    pieces = rows // 2 // half

    def place_of(p, k):
        return 2 * p + k if k < 2 else 2 * pieces if k < 4 else 2 * pieces + 1 + p

    scatters = [
        [
            remote("head", to, r.sent.at[pieces * k + p], r.back.at[pieces * k + p], r.o_send.at[0], r.o_recv.at[place_of(p, k)])
            for k, to in enumerate((across, along, across, along, along, across))
        ]
        for p in range(pieces)
    ]

    def put(p, k, value):
        r.sent[pieces * k + p] = value.astype(BF16)
        scatters[p][k].start()

    def piece(p):
        return slice(p * half, (p + 1) * half)

    def share(k, rs):
        return dot(r.g[rs, :], r.vw[k])

    def direct(k, source, rs):
        if source:
            value = share(source, rs)
        else:
            value = r.part[k] + dot(r.g[rs, ahead:], r.vw[0, ahead:, :])
        for p in range(pieces):
            put(p, k, value[piece(p), :])

    def joined(p):
        for k in (0, 1):
            scatters[p][k].wait_recv()
            put(p, 4 + k, r.part[k, piece(p), :] + r.back[pieces * k + p].astype(F32))

    direct(0, 0, upper_half)
    direct(1, 0, lower_half)
    spot = lax.broadcasted_iota(jnp.int32, (8, LANES), 0)
    squares = jnp.zeros((8, LANES), F32)
    for i in range(chunks):
        row = dot_nt(jnp.ones((8, LANES), F32), r.sums[chunk_rows(i), :], lax.Precision.HIGHEST)
        squares = jnp.where(spot == i, row, squares)
    r.squares[0] = squares
    small[0].start()
    direct(2, 1, upper_half)
    direct(3, 2, lower_half)
    r.part[0] = share(2, upper_half)
    r.part[1] = share(1, lower_half)
    for p in range(pieces):
        joined(p)
    small[0].wait_recv()
    r.squares[1] = r.squares[0] + r.others[0]
    small[1].start()
    own = r.y
    for rs in (upper_half, lower_half):
        own[rs, :depth] = share(3, rs)
    landing = r.back.at[2 * pieces : 4 * pieces]
    remote("head", across, landing, landing, r.o_send.at[0], r.o_recv.at[2 * pieces]).wait_recv()
    for k in (2, 3):
        base = (k - 2) * (rows // 2)
        for p in range(pieces):
            span = slice(base + p * half, base + (p + 1) * half)
            for i in range(depth // LANES):
                cols = slice(i * LANES, (i + 1) * LANES)
                own[span, cols] = own[span, cols] + r.back[pieces * k + p, :, cols].astype(F32)
    small[1].wait_recv()
    scale = lax.rsqrt((r.squares[1] + r.others[1]) / total + EPS)
    for i in range(chunks):
        r.sums[chunk_rows(i), :] = jnp.broadcast_to(scale[i : i + 1, :], (LANES, CHUNK)).T
    for p in range(pieces):
        landing = r.back.at[0:2]
        remote("head", across, landing, landing, r.o_send.at[0], r.o_recv.at[2 * pieces + 1 + p]).wait_recv()
        for k in (4, 5):
            base = (k - 4) * (rows // 2)
            span = slice(base + p * half, base + (p + 1) * half)
            for i in range(depth // LANES):
                cols = slice(i * LANES, (i + 1) * LANES)
                value = own[span, cols] + r.back[pieces * k + p, :, cols].astype(F32)
                out[span, cols] = (value * r.sums[span, :]).astype(BF16)

    for ref, send, recv in (
        (r.xt.at[:, : 3 * depth], r.g_send.at[0], r.g_recv.at[0]),
        (r.sent, r.o_send.at[0], r.o_recv.at[0]),
        (r.squares, r.q_send.at[0], r.q_recv.at[0]),
    ):
        remote("head", across, ref, ref, send, recv).wait_send()

    @pl.when(pos < chain - 1)
    def _():
        remote("seq", upper, r.leaving, r.leaving, r.c_send.at[0], r.c_recv.at[0]).wait_send()


def layer(chain, split, cores, tokens, resets, w_x, w_z, w_bc, w_dt, dt_bias, decay_rate, d_skip, norm_gain, w_out):
    rows, depth = tokens.shape
    width, heads, both = w_x.shape[1], w_dt.shape[1], w_bc.shape[1]
    blocks, pairs = rows // GROUP, width // LANES
    chunks = rows // CHUNK
    half = GROUP // 2
    vm, dma = pltpu.VMEM, pltpu.SemaphoreType.DMA
    scratch = dict(
        xt=vm((rows, 4 * depth), BF16),
        vx=vm((4 * depth, width), BF16),
        vz=vm((4 * depth, width), BF16),
        vb=vm((4 * depth, both), BF16),
        vw=vm((4, width, depth), BF16),
        wd=vm((LANES, 4 * depth), BF16),
        w_dt=vm((heads, 4 * depth), BF16),
        resets=vm((1, rows), jnp.int32),
        bias0=vm((1, heads), F32),
        rate0=vm((1, heads), F32),
        skip0=vm((1, heads), F32),
        bias=vm((1, LANES), F32),
        rate=vm((1, LANES), F32),
        skip=vm((1, LANES), F32),
        skips=vm((8, width), F32),
        gain0=vm((pairs, LANES), F32),
        gain=vm((1, width), F32),
        tri=vm((CHUNK, 3 * CHUNK), BF16),
        widen=vm((2 * LANES, width), BF16),
        mask=vm((chunks, CHUNK, CHUNK), F32),
        alone=vm((rows, LANES), F32),
        same=vm((rows, LANES), F32),
        open=vm((rows, LANES), F32),
        acc_x=vm((rows, width), F32),
        acc_z=vm((rows, width), F32),
        acc_m=vm((rows, both), F32),
        acc_s=vm((rows, LANES), F32),
        inner=vm((rows, width), BF16),
        gate=vm((rows, width), F32),
        mapped=vm((rows, both), BF16),
        turned=vm((blocks, NSTATE, GROUP), BF16),
        leave=vm((GROUP, 2 * LANES), BF16),
        ends=vm((8, 2 * LANES), BF16),
        through=vm((8, width), F32),
        mid=vm((NSTATE, width), F32),
        step=vm((GROUP, LANES), F32),
        before=vm((chunks + 1, LANES), F32),
        cum=vm((chunks, CHUNK, LANES), F32),
        cumt=vm((chunks, LANES, CHUNK), F32),
        stept=vm((chunks, LANES, CHUNK), F32),
        keep=vm((rows, 2 * LANES), BF16),
        enter=vm((rows, 2 * LANES), BF16),
        outer=vm((rows, 2 * LANES), BF16),
        score=vm((chunks, CHUNK, CHUNK), F32),
        state=vm((blocks, NSTATE, width), F32),
        arrived=vm((pairs, NSTATE, LANES), BF16),
        leaving=vm((pairs, NSTATE, LANES), BF16),
        y=vm((rows, width), F32),
        factor=vm((rows, width), F32),
        g=vm((rows, width), BF16),
        sums=vm((rows, LANES), F32),
        squares=vm((2, 8, LANES), F32),
        others=vm((2, 8, LANES), F32),
        part=vm((2, rows // 2, depth), F32),
        sent=vm((3 * rows // half, half, depth), BF16),
        back=vm((3 * rows // half, half, depth), BF16),
        small_load=dma((7,)),
        load=dma((9,)),
        g_send=dma((1,)),
        g_recv=dma((4 * blocks,)),
        c_send=dma((1,)),
        c_recv=dma((pairs,)),
        o_send=dma((1,)),
        o_recv=dma((3 * rows // 2 // half + 1,)),
        q_send=dma((1,)),
        q_recv=dma((2,)),
        go=pltpu.SemaphoreType.REGULAR((1,)),
    )
    return pl.pallas_call(
        functools.partial(kernel, chain, cores, float(width * split), tuple(scratch)),
        out_shape=pltpu.VMEM((rows, depth), BF16),
        in_specs=[ANY] * 11,
        out_specs=pl.BlockSpec(memory_space=pltpu.VMEM),
        scratch_shapes=list(scratch.values()),
        compiler_params=pltpu.CompilerParams(
            collective_id=0, has_side_effects=True, vmem_limit_bytes=60 * 1024 * 1024
        ),
    )(
        tokens, resets.reshape(1, rows), w_x, w_z, w_bc, w_dt.T, dt_bias.reshape(1, heads),
        decay_rate.reshape(1, heads), d_skip.reshape(1, heads), norm_gain.reshape(pairs, LANES), w_out,
    )


def solution(mesh):
    in_specs = (
        P(("batch", "seq"), "head"),
        P(("batch", "seq")),
        P(None, "head"),
        P(None, "head"),
        P(),
        P(None, "head"),
        P("head"),
        P("head"),
        P("head"),
        P("head"),
        P("head", None),
    )
    return jax.shard_map(
        functools.partial(layer, mesh.shape["seq"], mesh.shape["head"], mesh.shape["batch"]),
        mesh=mesh,
        in_specs=in_specs,
        out_specs=P(("batch", "seq"), "head"),
        check_vma=False,
    )
```
